32 devices in a mesh: model: 4 (over z), data: 2 (over y), stage: 4 (over x, core).
Axes of the slice: x: 2, y: 2, z: 4, core: 2. Of those that a mesh axis runs over, the one named last changes fastest.
Arguments:
- w_up: float32 [4, 768, 3072], P('stage', None, 'model')
- w_down: float32 [4, 3072, 768], P('stage', 'model')
- m_up: float32 [4, 768, 3072], P('stage', None, 'model')
- m_down: float32 [4, 3072, 768], P('stage', 'model')
- v_up: float32 [4, 768, 3072], P('stage', None, 'model')
- v_down: float32 [4, 3072, 768], P('stage', 'model')
- g_up: float32 [2, 4, 768, 3072], P('data', 'stage', None, 'model')
- g_down: float32 [2, 4, 3072, 768], P('data', 'stage', 'model')
- acts_last: bfloat16 [4, 2048, 768], P('stage', 'data')
- grad_out: bfloat16 [2048, 768], P('data')
- x_next: bfloat16 [16, 2048, 768], P(None, 'data')
- learn_rate: float32 [1], replicated
- max_norm: float32 [1], replicated
Outputs:
- output 1: float32 [4, 768, 3072], P('stage', None, 'model')
- output 2: float32 [4, 3072, 768], P('stage', 'model')
- output 3: float32 [4, 768, 3072], P('stage', None, 'model')
- output 4: float32 [4, 3072, 768], P('stage', 'model')
- output 5: float32 [4, 768, 3072], P('stage', None, 'model')
- output 6: float32 [4, 3072, 768], P('stage', 'model')
- output 7: bfloat16 [16, 2048, 768], P(None, 'data')
All inputs are finite; a program needn't handle non-finite values.
Results may differ from the reference program's by a relative error of at most 0.00895596.
Values are sent between devices in bfloat16 or wider.
A program may use at most 1 GiB of HBM per device.

```python
import jax
import jax.numpy as jnp
from jax import lax

STAGES = 4
REPLICAS = 2
D_MODEL = 768
FF_WIDTH = 3072
MICRO_ROWS = 1024
NEXT_MICRO = 16
ADAM_STEP = 10
BETA_ONE = 0.9
BETA_TWO = 0.95
ADAM_EPS = 1e-8
WEIGHT_DECAY = 0.1
NORM_EPS = 1e-6
ALL_ROWS = REPLICAS * MICRO_ROWS


def gelu_vjp(pre_act, upstream):
    pull_back = jax.vjp(jax.nn.gelu, pre_act)[1]
    return pull_back(upstream)[0]


def stage_apply(acts_in, up_bf, down_bf):
    pre_act = jnp.dot(acts_in, up_bf, preferred_element_type=jnp.float32)
    hidden = jax.nn.gelu(pre_act).astype(jnp.bfloat16)
    branch = jnp.dot(hidden, down_bf, preferred_element_type=jnp.float32)
    return (acts_in.astype(jnp.float32) + branch).astype(jnp.bfloat16)


def averaged_grads(w_up, w_down, g_up, g_down, acts_last, grad_out):
    def back_step(upstream, layer_in):
        up_bf, down_bf, acts_in = layer_in
        pre_act = jnp.dot(acts_in, up_bf, preferred_element_type=jnp.float32)
        hidden = jax.nn.gelu(pre_act).astype(jnp.bfloat16)
        grad_down = jnp.dot(hidden.T, upstream, preferred_element_type=jnp.float32)
        grad_hid = jnp.dot(upstream, down_bf.T, preferred_element_type=jnp.float32)
        grad_pre = gelu_vjp(pre_act, grad_hid).astype(jnp.bfloat16)
        grad_up = jnp.dot(acts_in.T, grad_pre, preferred_element_type=jnp.float32)
        back_in = jnp.dot(grad_pre, up_bf.T, preferred_element_type=jnp.float32)
        grad_in = (upstream.astype(jnp.float32) + back_in).astype(jnp.bfloat16)
        return grad_in, (grad_up, grad_down)
    layer_all = (w_up.astype(jnp.bfloat16), w_down.astype(jnp.bfloat16), acts_last)
    grad_pair = lax.scan(back_step, grad_out, layer_all, reverse=True)[1]
    mean_up = (jnp.sum(g_up, axis=0) + grad_pair[0]) / REPLICAS
    mean_down = (jnp.sum(g_down, axis=0) + grad_pair[1]) / REPLICAS
    return mean_up, mean_down


def adamw_update(weight, moment_one, moment_two, grad_step, step_rate):
    mom_new = BETA_ONE * moment_one + (1.0 - BETA_ONE) * grad_step
    sec_new = BETA_TWO * moment_two + (1.0 - BETA_TWO) * grad_step * grad_step
    one_corr = 1.0 - BETA_ONE ** ADAM_STEP
    two_corr = 1.0 - BETA_TWO ** ADAM_STEP
    direction = (mom_new / one_corr) / (jnp.sqrt(sec_new / two_corr) + ADAM_EPS)
    weight_new = weight - step_rate * (direction + WEIGHT_DECAY * weight)
    return weight_new, mom_new, sec_new


def forward_all(up_bf, down_bf, x_next):
    def one_micro(acts_in):
        def fwd_step(acts_carry, layer_in):
            return stage_apply(acts_carry, layer_in[0], layer_in[1]), None
        return lax.scan(fwd_step, acts_in, (up_bf, down_bf))[0]
    return lax.map(one_micro, x_next)


def setup_inputs(seed: int = 0) -> dict:
    key_list = jax.random.split(jax.random.key(seed), 13)
    up_scale = D_MODEL ** -0.5
    down_scale = FF_WIDTH ** -0.5
    grad_scale = MICRO_ROWS ** 0.5
    w_up = jax.random.normal(key_list[0], (STAGES, D_MODEL, FF_WIDTH), jnp.float32) * up_scale
    w_down = jax.random.normal(key_list[1], (STAGES, FF_WIDTH, D_MODEL), jnp.float32) * down_scale
    g_up = jax.random.normal(key_list[2], (REPLICAS, STAGES, D_MODEL, FF_WIDTH), jnp.float32) * (0.3 * grad_scale)
    g_down = jax.random.normal(key_list[3], (REPLICAS, STAGES, FF_WIDTH, D_MODEL), jnp.float32) * (0.5 * grad_scale)
    acts_last = jax.random.normal(key_list[4], (STAGES, ALL_ROWS, D_MODEL), jnp.float32).astype(jnp.bfloat16)
    grad_out = jax.random.normal(key_list[5], (ALL_ROWS, D_MODEL), jnp.float32).astype(jnp.bfloat16)
    x_next = jax.random.normal(key_list[6], (NEXT_MICRO, ALL_ROWS, D_MODEL), jnp.float32).astype(jnp.bfloat16)
    learn_rate = jax.random.uniform(key_list[7], (1,), jnp.float32, 0.1, 0.25) * up_scale
    mean_up, mean_down = averaged_grads(w_up, w_down, g_up, g_down, acts_last, grad_out)
    grad_norm = jnp.sqrt(jnp.sum(mean_up * mean_up) + jnp.sum(mean_down * mean_down))
    clip_frac = jax.random.uniform(key_list[8], (1,), jnp.float32, 0.35, 0.65)
    max_norm = clip_frac * grad_norm
    up_rms = clip_frac[0] * jnp.sqrt(jnp.mean(mean_up * mean_up))
    down_rms = clip_frac[0] * jnp.sqrt(jnp.mean(mean_down * mean_down))
    m_up = jax.random.normal(key_list[9], w_up.shape, jnp.float32) * (0.1 * up_rms)
    m_down = jax.random.normal(key_list[10], w_down.shape, jnp.float32) * (0.1 * down_rms)
    v_up = (0.5 + jax.random.uniform(key_list[11], w_up.shape, jnp.float32)) * (0.02 * up_rms * up_rms)
    v_down = (0.5 + jax.random.uniform(key_list[12], w_down.shape, jnp.float32)) * (0.02 * down_rms * down_rms)
    return {'w_up': w_up, 'w_down': w_down, 'm_up': m_up, 'm_down': m_down, 'v_up': v_up, 'v_down': v_down, 'g_up': g_up, 'g_down': g_down, 'acts_last': acts_last, 'grad_out': grad_out, 'x_next': x_next, 'learn_rate': learn_rate, 'max_norm': max_norm}


def reference(w_up, w_down, m_up, m_down, v_up, v_down, g_up, g_down, acts_last, grad_out, x_next, learn_rate, max_norm):
    mean_up, mean_down = averaged_grads(w_up, w_down, g_up, g_down, acts_last, grad_out)
    norm_sq = jnp.sum(mean_up * mean_up) + jnp.sum(mean_down * mean_down)
    clip_scale = jnp.minimum(1.0, max_norm[0] / (jnp.sqrt(norm_sq) + NORM_EPS))
    up_new, up_mom, up_sec = adamw_update(w_up, m_up, v_up, clip_scale * mean_up, learn_rate[0])
    down_new, down_mom, down_sec = adamw_update(w_down, m_down, v_down, clip_scale * mean_down, learn_rate[0])
    y_next = forward_all(up_new.astype(jnp.bfloat16), down_new.astype(jnp.bfloat16), x_next)
    return (up_new, down_new, up_mom, down_mom, up_sec, down_sec, y_next)
```

```python
import functools

import jax
import jax.numpy as jnp
from jax import lax
from jax.experimental import pallas as pl
from jax.experimental.pallas import tpu as pltpu
from jax.sharding import PartitionSpec as P

ADAM_STEP = 10
BETA_ONE = 0.9
BETA_TWO = 0.95
ADAM_EPS = 1e-8
WEIGHT_DECAY = 0.1
NORM_EPS = 1e-6
CONTRACT_LAST = (((1,), (1,)), ((), ()))
CONTRACT_FIRST = (((0,), (0,)), ((), ()))
F32 = jnp.float32
BF16 = jnp.bfloat16


def gelu_vjp(pre_act, upstream):
    pull_back = jax.vjp(jax.nn.gelu, pre_act)[1]
    return pull_back(upstream)[0]


def adamw_update(weight, moment_one, moment_two, grad_step, step_rate):
    mom_new = BETA_ONE * moment_one + (1.0 - BETA_ONE) * grad_step
    sec_new = BETA_TWO * moment_two + (1.0 - BETA_TWO) * grad_step * grad_step
    one_corr = 1.0 - BETA_ONE ** ADAM_STEP
    two_corr = 1.0 - BETA_TWO ** ADAM_STEP
    direction = (mom_new / one_corr) / (jnp.sqrt(sec_new / two_corr) + ADAM_EPS)
    weight_new = weight - step_rate * (direction + WEIGHT_DECAY * weight)
    return weight_new, mom_new, sec_new


def dot(left, right, dims=None):
    if dims is None:
        return jnp.dot(left, right, preferred_element_type=F32)
    return lax.dot_general(left, right, dims, preferred_element_type=F32)


class Net:
    def __init__(self):
        self.z = lax.axis_index('model')
        self.y = lax.axis_index('data')
        self.s = lax.axis_index('stage')
        self.y_other = 1 - self.y
        self.s_across = lax.rem(self.s + 2, 4)
        self.s_sibling = self.s + 1 - 2 * lax.rem(self.s, 2)
        self.sends = []

    def send(self, src, dst, send_sem, recv_sem, to):
        return pltpu.make_async_remote_copy(src_ref=src, dst_ref=dst, send_sem=send_sem, recv_sem=recv_sem, device_id=to, device_id_type=pl.DeviceIdType.MESH)


def when_all(conds, body):
    cond = None
    for c in conds:
        if c is not None:
            cond = c if cond is None else cond & c
    if cond is None:
        body()
    else:
        pl.when(cond)(body)


def side_of(z, n_model, d, side):
    if d == 0:
        return z, None
    if side == 0:
        return lax.max(z - d, 0), z - d >= 0
    return lax.min(z + d, n_model - 1), z + d < n_model


def chain_kernel(n_model, own, acts, grad, gathered, wfull, pre, gbuf, obuf, wsend, wrecv, ysend, yrecv, gsend, grecv, csend, crecv):
    net = Net()
    z, y, s = net.z, net.y, net.s
    n_stage = 4
    half, width = own.shape[2], own.shape[3]
    pend = []

    def z_copy(zs, mat, up, src):
        to = z + 1 if up else z - 1
        return net.send(src, wfull.at[zs, y, mat], wsend.at[int(up), zs, mat], wrecv.at[zs, mat], {'model': to})

    def y_copy(zs, mat):
        return net.send(wfull.at[zs, y, mat], wfull.at[zs, y, mat], ysend.at[zs, mat], yrecv.at[zs, mat], {'data': net.y_other})

    for mat in range(2):
        own_half = own.at[mat, y]
        for up in (False, True):
            cond = (z < n_model - 1) if up else (z > 0)
            def start(mat=mat, up=up, own_half=own_half):
                z_copy(z, mat, up, own_half).start()
            pl.when(cond)(start)
    for mat in range(2):
        for h in range(2):
            wfull[z, h, mat] = own[mat, h]

    def use(zs, mat):
        return wfull.at[zs, :, mat]

    for d in range(1, n_model):
        for mat in range(2):
            for side in range(2):
                zs, ok = side_of(z, n_model, d, side)
                up = side == 0
                room = (z < n_model - 1) if up else (z > 0)
                def take(zs=zs, mat=mat, up=up):
                    z_copy(zs, mat, up, wfull.at[zs, y, mat]).wait_recv()
                    y_copy(zs, mat).start()
                when_all([ok], take)
                def forward(zs=zs, mat=mat, up=up):
                    z_copy(zs, mat, up, wfull.at[zs, y, mat]).start()
                when_all([ok, room], forward)
    for d in range(1, n_model):
        for mat in range(2):
            for side in range(2):
                zs, ok = side_of(z, n_model, d, side)
                def take_y(zs=zs, mat=mat):
                    net.send(wfull.at[zs, net.y_other, mat], wfull.at[zs, net.y_other, mat], ysend.at[zs, mat], yrecv.at[zs, mat], {'data': net.y_other}).wait_recv()
                when_all([ok], take_y)

    def pre_body(j, _):
        up_w = wfull[j, :, 0].reshape(2 * half, width)
        pre[j] = dot(acts[...], up_w)
        return 0

    lax.fori_loop(0, n_model, pre_body, 0)

    g_in = net.send(obuf, gbuf, csend.at[0], crecv.at[0], {'stage': lax.max(s - 1, 0)})

    def g_copy(zs, up, src):
        to = z + 1 if up else z - 1
        return net.send(src, gathered.at[zs], gsend.at[int(up), zs], grecv.at[zs], {'model': to})

    @pl.when(s == n_stage - 1)
    def _():
        gbuf[...] = grad[...]

    @pl.when(s < n_stage - 1)
    def _():
        g_in.wait_recv()
        for up in (False, True):
            cond = (z < n_model - 1) if up else (z > 0)
            def start(up=up):
                g_copy(z, up, gbuf).start()
            pl.when(cond)(start)

    @pl.when(s > 0)
    def _():
        def back_body(j, total):
            down_w = wfull[j, :, 1].reshape(2 * half, width)
            up_w = wfull[j, :, 0].reshape(2 * half, width)
            grad_hid = dot(gbuf[...], down_w, CONTRACT_LAST)
            grad_pre = gelu_back(pre[j], grad_hid).astype(BF16)
            return total + dot(grad_pre, up_w, CONTRACT_LAST)

        total = lax.fori_loop(0, n_model, back_body, jnp.zeros(gbuf.shape, F32))
        obuf[...] = (gbuf[...].astype(F32) + total).astype(BF16)
        g_in.start()

    gathered[z] = gbuf[...]

    @pl.when(s < n_stage - 1)
    def _():
        for d in range(1, n_model):
            for side in range(2):
                zs, ok = side_of(z, n_model, d, side)
                up = side == 0
                room = (z < n_model - 1) if up else (z > 0)
                def take(zs=zs, up=up):
                    g_copy(zs, up, gathered.at[zs]).wait_recv()
                when_all([ok], take)
                def forward(zs=zs, up=up):
                    g_copy(zs, up, gathered.at[zs]).start()
                when_all([ok, room], forward)

    for d in range(n_model):
        for side in range(2 if d else 1):
            zs, ok = side_of(z, n_model, d, side)
            for up in (False, True):
                if d and up != (side == 0):
                    continue
                room = (z < n_model - 1) if up else (z > 0)
                for mat in range(2):
                    def drain(zs=zs, up=up, mat=mat):
                        z_copy(zs, mat, up, wfull.at[zs, y, mat]).wait_send()
                    when_all([ok, room], drain)
                def drain_g(zs=zs, up=up):
                    g_copy(zs, up, gathered.at[zs]).wait_send()
                when_all([ok, room, s < n_stage - 1], drain_g)
            if d:
                for mat in range(2):
                    def drain_y(zs=zs, mat=mat):
                        y_copy(zs, mat).wait_send()
                    when_all([ok], drain_y)

    @pl.when(s > 0)
    def _():
        g_in.wait_send()


def gelu_back(pre_act, upstream):
    scale = 0.7978845608028654
    cubic = 0.044715
    inner = scale * (pre_act + cubic * pre_act * pre_act * pre_act)
    tanh = jnp.tanh(inner)
    slope = scale * (1.0 + 3.0 * cubic * pre_act * pre_act)
    return upstream * (0.5 * (1.0 + tanh) + 0.5 * pre_act * (1.0 - tanh * tanh) * slope)


VMEM_SPEC = pl.BlockSpec(memory_space=pltpu.VMEM)
ANY_SPEC = pl.BlockSpec(memory_space=pl.ANY)
DMA = pltpu.SemaphoreType.DMA


def backward_rows(own, acts, grad, n_model):
    rows, width = acts.shape
    half = own.shape[2]
    return pl.pallas_call(
        functools.partial(chain_kernel, n_model),
        out_shape=jax.ShapeDtypeStruct((n_model, rows, width), BF16),
        in_specs=[VMEM_SPEC] * 3,
        out_specs=VMEM_SPEC,
        scratch_shapes=[
            pltpu.VMEM((n_model, 2, 2, half, width), BF16),
            pltpu.VMEM((n_model, rows, 2 * half), F32),
            pltpu.VMEM((rows, width), BF16),
            pltpu.VMEM((rows, width), BF16),
            DMA((2, n_model, 2)), DMA((n_model, 2)), DMA((n_model, 2)), DMA((n_model, 2)),
            DMA((2, n_model)), DMA((n_model,)), DMA((1,)), DMA((1,)),
        ],
        compiler_params=pltpu.CompilerParams(has_side_effects=True, vmem_limit_bytes=48 * 1024 * 1024),
        name='chain',
    )(own, acts, grad)


def weights_kernel(n_model, own, new, zsend, xsend, ysend, csend, recv, local):
    net = Net()
    z, y, s = net.z, net.y, net.s
    c = lax.rem(s, 2)

    def slot(ss, zs, ys, mat):
        return new.at[ss, zs, ys, mat]

    def copy(src, ss, zs, ys, mat, sem, to):
        return net.send(src, slot(ss, zs, ys, mat), sem, recv.at[ss, zs, ys, mat], to)

    def go(kind, ss, zs, ys, mat, src=None):
        src = slot(ss, zs, ys, mat) if src is None else src
        if kind == 'up':
            return copy(src, ss, zs, ys, mat, zsend.at[1, zs, mat], {'model': z + 1})
        if kind == 'down':
            return copy(src, ss, zs, ys, mat, zsend.at[0, zs, mat], {'model': z - 1})
        if kind == 'x':
            return copy(src, ss, zs, ys, mat, xsend.at[zs, ys, mat], {'stage': net.s_across})
        if kind == 'y':
            return copy(src, ss, zs, ys, mat, ysend.at[ss // 2, zs, mat], {'data': net.y_other})
        return copy(src, ss, zs, ys, mat, csend.at[ss // 2, zs, ys, mat], {'stage': net.s_sibling})

    def arrive(ss, zs, ys, mat):
        go('c', ss, zs, ys, mat).wait_recv()

    def first(d, side, mat, act):
        zs, ok = side_of(z, n_model, d, side)
        src = own.at[mat] if d == 0 else None
        for kind in ('up', 'down'):
            if d and kind != ('up' if side == 0 else 'down'):
                continue
            room = (z < n_model - 1) if kind == 'up' else (z > 0)
            when_all([ok, room], lambda kind=kind: act(go(kind, s, zs, y, mat, src)))
        def rest():
            for kind in ('x', 'y', 'c'):
                act(go(kind, s, zs, y, mat, src))
        when_all([ok], rest)

    def beside(mat, zs):
        return (s, zs, net.y_other, mat) if mat == 0 else (net.s_across, zs, y, mat)

    def second(d, side, mat, act):
        zs, ok = side_of(z, n_model, d, side)
        ss, ys, kind = (net.s_across, y, 'y') if mat == 0 else (s, net.y_other, 'x')
        def rest():
            act(go(kind, ss, zs, ys, mat))
            act(go('c', ss, zs, ys, mat))
            act(go('c', *beside(mat, zs)))
        when_all([ok], rest)

    def third(d, side, mat, act):
        zs, ok = side_of(z, n_model, d, side)
        when_all([ok], lambda: act(go('c', net.s_across, zs, net.y_other, mat)))

    def start(copy):
        copy.start()

    def end(copy):
        copy.wait_send()

    def step(level, d):
        for side in range(2 if d else 1):
            for mat in range(2):
                zs, ok = side_of(z, n_model, d, side)
                if level == 0:
                    if d:
                        when_all([ok], lambda: arrive(s, zs, y, mat))
                    first(d, side, mat, start)
                elif level == 1:
                    ss, ys = (net.s_across, y) if mat == 0 else (s, net.y_other)
                    def both():
                        arrive(ss, zs, ys, mat)
                        arrive(*beside(mat, zs))
                    when_all([ok], both)
                    second(d, side, mat, start)
                else:
                    when_all([ok], lambda: arrive(net.s_across, zs, net.y_other, mat))
                    third(d, side, mat, start)

    mine = pltpu.make_async_copy(own, new.at[s, z, y], local.at[0])
    mine.start()
    for level, d in ((0, 0), (0, 1), (1, 0), (0, 2), (1, 1), (2, 0), (0, 3), (1, 2), (2, 1), (1, 3), (2, 2), (2, 3)):
        step(level, d)
    for ss in (net.s_sibling, lax.rem(net.s_sibling + 2, 4)):
        for zs in range(n_model):
            for ys in range(2):
                for mat in range(2):
                    arrive(ss, zs, ys, mat)
    for d in range(n_model):
        for side in range(2 if d else 1):
            for mat in range(2):
                first(d, side, mat, end)
                second(d, side, mat, end)
                third(d, side, mat, end)
    mine.wait()


def gather_weights(own, n_stage, n_model, n_data):
    n_mat, half, width = own.shape
    return pl.pallas_call(
        functools.partial(weights_kernel, n_model),
        out_shape=jax.ShapeDtypeStruct((n_stage, n_model, n_data, n_mat, half, width), BF16),
        in_specs=[VMEM_SPEC],
        out_specs=ANY_SPEC,
        scratch_shapes=[
            DMA((2, n_model, 2)), DMA((n_model, 2, 2)), DMA((2, n_model, 2)), DMA((2, n_model, 2, 2)),
            DMA((n_stage, n_model, n_data, n_mat)), DMA((1,)),
        ],
        compiler_params=pltpu.CompilerParams(has_side_effects=True),
        name='weights',
    )(own)


def out_kernel(n_model, cut, own, out, zsend, xsend, csend, recv, local):
    net = Net()
    z, s = net.z, net.s
    rows = own.shape[0]
    parts = (pl.ds(0, cut), pl.ds(cut, rows - cut))

    def slot(ss, zs, part):
        return out.at[ss * n_model + zs, parts[part]]

    def go(kind, ss, zs, part, src=None):
        src = slot(ss, zs, part) if src is None else src
        if kind == 'up':
            sem, to = zsend.at[1, ss // 2, zs, part], {'model': z + 1}
        elif kind == 'down':
            sem, to = zsend.at[0, ss // 2, zs, part], {'model': z - 1}
        elif kind == 'x':
            sem, to = xsend.at[zs, part], {'stage': net.s_across}
        else:
            sem, to = csend.at[ss // 2, zs, part], {'stage': net.s_sibling}
        return net.send(src, slot(ss, zs, part), sem, recv.at[ss, zs, part], to)

    def arrive(ss, zs, part):
        go('c', ss, zs, part).wait_recv()

    def along_z(ss, d, side, part, act, src=None):
        zs, ok = side_of(z, n_model, d, side)
        for kind in ('up', 'down'):
            if d and kind != ('up' if side == 0 else 'down'):
                continue
            room = (z < n_model - 1) if kind == 'up' else (z > 0)
            when_all([ok, room], lambda kind=kind: act(go(kind, ss, zs, part, src)))

    def big(d, side, act):
        zs, ok = side_of(z, n_model, d, side)
        src = own.at[parts[0]] if d == 0 else None
        along_z(s, d, side, 0, act, src)
        def rest():
            act(go('x', s, zs, 0, src))
            act(go('c', s, zs, 0, src))
        when_all([ok], rest)

    def big_across(d, side, act):
        zs, ok = side_of(z, n_model, d, side)
        when_all([ok], lambda: act(go('c', net.s_across, zs, 0)))

    def small(ss, d, side, act, src=None):
        zs, ok = side_of(z, n_model, d, side)
        along_z(ss, d, side, 1, act, src)
        when_all([ok], lambda: act(go('c', ss, zs, 1, src)))

    def start(copy):
        copy.start()

    def end(copy):
        copy.wait_send()

    def sides(d):
        return range(2 if d else 1)

    mine = pltpu.make_async_copy(own, out.at[s * n_model + z], local.at[0])
    mine.start()
    go('x', s, z, 1, own.at[parts[1]]).start()
    big(0, 0, start)
    small(s, 0, 0, start, own.at[parts[1]])
    arrive(net.s_across, z, 1)
    small(net.s_across, 0, 0, start)
    for d in range(1, n_model):
        for side in sides(d):
            zs, ok = side_of(z, n_model, d, side)
            when_all([ok], lambda: arrive(s, zs, 0))
            big(d, side, start)
        for ss in (s, net.s_across):
            for side in sides(d):
                zs, ok = side_of(z, n_model, d, side)
                when_all([ok], lambda: arrive(ss, zs, 1))
                small(ss, d, side, start)
        for side in sides(d - 1):
            zs, ok = side_of(z, n_model, d - 1, side)
            when_all([ok], lambda: arrive(net.s_across, zs, 0))
            big_across(d - 1, side, start)
    for side in sides(n_model - 1):
        zs, ok = side_of(z, n_model, n_model - 1, side)
        when_all([ok], lambda: arrive(net.s_across, zs, 0))
        big_across(n_model - 1, side, start)
    for ss in (net.s_sibling, lax.rem(net.s_sibling + 2, 4)):
        for zs in range(n_model):
            for part in range(2):
                arrive(ss, zs, part)
    go('x', s, z, 1, own.at[parts[1]]).wait_send()
    for d in range(n_model):
        for side in sides(d):
            big(d, side, end)
            big_across(d, side, end)
            small(s, d, side, end, own.at[parts[1]] if d == 0 else None)
            small(net.s_across, d, side, end)
    mine.wait()


def gather_out(own, n_stage, n_model):
    rows, width = own.shape
    cut = rows * 7 // 8
    return pl.pallas_call(
        functools.partial(out_kernel, n_model, cut),
        out_shape=jax.ShapeDtypeStruct((n_stage * n_model, rows, width), BF16),
        in_specs=[VMEM_SPEC],
        out_specs=ANY_SPEC,
        scratch_shapes=[
            DMA((2, 2, n_model, 2)), DMA((n_model, 2)), DMA((2, n_model, 2)),
            DMA((n_stage, n_model, 2)), DMA((1,)),
        ],
        compiler_params=pltpu.CompilerParams(has_side_effects=True),
        name='gather_out',
    )(own)


def norm_kernel(n_stage, n_data, n_model, part, total, slots, send_sem, recv_sem):
    net = Net()
    z, y, s = net.z, net.y, net.s
    count = n_stage * n_data * n_model
    me = (s * n_data + y) * n_model + z

    def copy(k):
        other = lax.rem(me + k, count)
        to = {'model': lax.rem(other, n_model), 'data': lax.rem(other // n_model, n_data), 'stage': other // (n_model * n_data)}
        return net.send(part, slots.at[me], send_sem.at[k], recv_sem.at[me], to)

    def from_other(k):
        other = lax.rem(me + k, count)
        return net.send(part, slots.at[other], send_sem.at[k], recv_sem.at[other], {'model': z, 'data': y, 'stage': lax.rem(s + 1, n_stage)})

    for k in range(1, count):
        copy(k).start()
    slots[me] = part[...]
    for k in range(1, count):
        from_other(k).wait_recv()
    total[...] = jnp.sum(slots[...], axis=0)
    for k in range(1, count):
        copy(k).wait_send()


def total_sum(part, n_stage, n_data, n_model):
    count = n_stage * n_data * n_model
    tile = pl.pallas_call(
        functools.partial(norm_kernel, n_stage, n_data, n_model),
        out_shape=jax.ShapeDtypeStruct((8, 128), F32),
        in_specs=[VMEM_SPEC],
        out_specs=VMEM_SPEC,
        scratch_shapes=[pltpu.VMEM((count, 8, 128), F32), DMA((count,)), DMA((count,))],
        compiler_params=pltpu.CompilerParams(has_side_effects=True),
        name='norm',
    )(part)
    return jnp.sum(tile)


def mlp_kernel(rows_step, acts, up, down, out, cur, total):
    p, j = pl.program_id(0), pl.program_id(1)
    rows, width = cur.shape

    @pl.when((p == 0) & (j == 0))
    def _():
        cur[...] = acts[...]

    up_w = up[0, 0, :, 0].reshape(width, width)
    down_w = down[0, 0, :, 0].reshape(width, width)
    for r in range(rows // rows_step):
        at = pl.ds(r * rows_step, rows_step)
        hid = jax.nn.gelu(dot(cur[at, :], up_w)).astype(BF16)
        part = dot(hid, down_w)

        @pl.when(j == 0)
        def _():
            total[at, :] = part

        @pl.when(j > 0)
        def _():
            total[at, :] += part

    @pl.when(j == pl.num_programs(1) - 1)
    def _():
        cur[...] = (cur[...].astype(F32) + total[...]).astype(BF16)

    @pl.when((p == pl.num_programs(0) - 1) & (j == pl.num_programs(1) - 1))
    def _():
        out[...] = cur[...]


def forward_rows(acts, new):
    n_stage, n_model, n_data, _, half, width = new.shape
    rows = acts.shape[0]
    def spec(mat):
        return pl.BlockSpec((1, 1, n_data, 1, half, width), lambda p, j: (p, j, 0, mat, 0, 0))
    whole = pl.BlockSpec((rows, width), lambda p, j: (0, 0))
    return pl.pallas_call(
        functools.partial(mlp_kernel, 256),
        out_shape=jax.ShapeDtypeStruct((rows, width), BF16),
        grid=(n_stage, n_model),
        in_specs=[whole, spec(0), spec(1)],
        out_specs=whole,
        scratch_shapes=[pltpu.VMEM((rows, width), BF16), pltpu.VMEM((rows, width), F32)],
        compiler_params=pltpu.CompilerParams(dimension_semantics=('arbitrary', 'arbitrary'), vmem_limit_bytes=40 * 1024 * 1024),
        cost_estimate=pl.CostEstimate(flops=4 * n_stage * rows * width * width * n_model, bytes_accessed=2 * new.size, transcendentals=n_stage * n_model * rows * width),
        name='forward',
    )(acts, new, new)


def solution(mesh):
    n_stage = mesh.shape['stage']
    n_data = mesh.shape['data']
    n_model = mesh.shape['model']
    swap = [(0, 1), (1, 0)]
    up_spec = P('stage', None, 'model')
    down_spec = P('stage', 'model', None)
    row_spec = P(None, 'data', None)
    in_specs = (up_spec, down_spec, up_spec, down_spec, up_spec, down_spec, P('data', 'stage', None, 'model'), P('data', 'stage', 'model', None), P('stage', 'data', None), P('data', None), row_spec, P(None), P(None))
    out_specs = (up_spec, down_spec, up_spec, down_spec, up_spec, down_spec, row_spec)

    def device_step(w_up, w_down, m_up, m_down, v_up, v_down, g_up, g_down, acts_last, grad_out, x_next, learn_rate, max_norm):
        stage_id = lax.axis_index('stage')
        model_id = lax.axis_index('model')
        data_id = lax.axis_index('data')
        acts_in = acts_last[0]
        w_up, w_down, m_up, m_down, v_up, v_down = (t[0] for t in (w_up, w_down, m_up, m_down, v_up, v_down))
        g_up, g_down = g_up[0, 0], g_down[0, 0]
        d_model, ff_local = w_up.shape
        rows = acts_in.shape[0]
        row_part = rows // n_model
        half = d_model // n_data
        up_bf = w_up.astype(BF16)
        down_bf = w_down.astype(BF16)

        def half_of(arr, which):
            return lax.dynamic_slice_in_dim(arr, which * half, half, 0)

        own = jnp.stack([up_bf, down_bf]).reshape(2, n_data, half, d_model)
        acts_part = lax.dynamic_slice_in_dim(acts_in, model_id * row_part, row_part, 0)
        grad_part = lax.dynamic_slice_in_dim(grad_out, model_id * row_part, row_part, 0)
        gathered = backward_rows(own, acts_part, grad_part, n_model).reshape(rows, d_model)
        grad_full = jnp.where(stage_id == n_stage - 1, grad_out, gathered)

        pre_act = dot(acts_in, up_bf)
        hidden = jax.nn.gelu(pre_act).astype(BF16)
        grad_hid = dot(grad_full, down_bf, CONTRACT_LAST)
        grad_pre = gelu_vjp(pre_act, grad_hid).astype(BF16)
        sum_up = g_up + dot(acts_in, grad_pre, CONTRACT_FIRST)
        sum_down = g_down + dot(hidden, grad_full, CONTRACT_FIRST)
        got_up = lax.ppermute(half_of(sum_up, 1 - data_id), 'data', swap)
        got_down = lax.ppermute(half_of(sum_down, 1 - data_id), 'data', swap)
        mean_up = (half_of(sum_up, data_id) + got_up) / n_data
        mean_down = (half_of(sum_down, data_id) + got_down) / n_data
        sq = mean_up * mean_up + mean_down * mean_down
        norm_sq = total_sum(jnp.sum(sq.reshape(-1, 8, d_model // 128, 128), axis=(0, 2)), n_stage, n_data, n_model)
        clip = jnp.minimum(1.0, max_norm[0] / (jnp.sqrt(norm_sq) + NORM_EPS))
        step_rate = learn_rate[0]

        up_half = adamw_update(half_of(w_up, data_id), half_of(m_up, data_id), half_of(v_up, data_id), clip * mean_up, step_rate)[0]
        down_half = adamw_update(half_of(w_down, data_id), half_of(m_down, data_id), half_of(v_down, data_id), clip * mean_down, step_rate)[0]
        new = gather_weights(jnp.stack([up_half.astype(BF16), down_half.astype(BF16)]), n_stage, n_model, n_data)

        other_up = lax.ppermute(mean_up, 'data', swap)
        other_down = lax.ppermute(mean_down, 'data', swap)

        def join(mine, other):
            first = jnp.where(data_id == 0, mine, other)
            second = jnp.where(data_id == 0, other, mine)
            return jnp.concatenate([first, second], axis=0)

        up_w, up_m, up_v = adamw_update(w_up, m_up, v_up, clip * join(mean_up, other_up), step_rate)
        down_w, down_m, down_v = adamw_update(w_down, m_down, v_down, clip * join(mean_down, other_down), step_rate)

        acts_cur = lax.dynamic_index_in_dim(x_next, stage_id * n_model + model_id, 0, keepdims=False)
        y_next = gather_out(forward_rows(acts_cur, new), n_stage, n_model)
        return (up_w[None], down_w[None], up_m[None], down_m[None], up_v[None], down_v[None], y_next)

    return jax.shard_map(device_step, mesh=mesh, in_specs=in_specs, out_specs=out_specs, check_vma=False)
```

```python
import functools

import jax
import jax.numpy as jnp
from jax import lax
from jax.experimental import pallas as pl
from jax.experimental.pallas import tpu as pltpu
from jax.sharding import PartitionSpec as P

ADAM_STEP = 10
BETA_ONE = 0.9
BETA_TWO = 0.95
ADAM_EPS = 1e-8
WEIGHT_DECAY = 0.1
NORM_EPS = 1e-6
CONTRACT_LAST = (((1,), (1,)), ((), ()))
CONTRACT_FIRST = (((0,), (0,)), ((), ()))
F32 = jnp.float32
BF16 = jnp.bfloat16


def adamw_update(weight, moment_one, moment_two, grad_step, step_rate):
    mom_new = BETA_ONE * moment_one + (1.0 - BETA_ONE) * grad_step
    sec_new = BETA_TWO * moment_two + (1.0 - BETA_TWO) * grad_step * grad_step
    one_corr = 1.0 - BETA_ONE ** ADAM_STEP
    two_corr = 1.0 - BETA_TWO ** ADAM_STEP
    direction = (mom_new / one_corr) / (jnp.sqrt(sec_new / two_corr) + ADAM_EPS)
    weight_new = weight - step_rate * (direction + WEIGHT_DECAY * weight)
    return weight_new, mom_new, sec_new


def dot(left, right, dims=None):
    if dims is None:
        return jnp.dot(left, right, preferred_element_type=F32)
    return lax.dot_general(left, right, dims, preferred_element_type=F32)


class Net:
    def __init__(self):
        self.z = lax.axis_index('model')
        self.y = lax.axis_index('data')
        self.s = lax.axis_index('stage')
        self.y_other = 1 - self.y
        self.s_across = lax.rem(self.s + 2, 4)
        self.s_sibling = self.s + 1 - 2 * lax.rem(self.s, 2)
        self.sends = []

    def send(self, src, dst, send_sem, recv_sem, to):
        return pltpu.make_async_remote_copy(src_ref=src, dst_ref=dst, send_sem=send_sem, recv_sem=recv_sem, device_id=to, device_id_type=pl.DeviceIdType.MESH)


def when_all(conds, body):
    cond = None
    for c in conds:
        if c is not None:
            cond = c if cond is None else cond & c
    if cond is None:
        body()
    else:
        pl.when(cond)(body)


def side_of(z, n_model, d, side):
    if d == 0:
        return z, None
    if side == 0:
        return lax.max(z - d, 0), z - d >= 0
    return lax.min(z + d, n_model - 1), z + d < n_model


def gelu_parts(pre_act):
    scale = 0.7978845608028654
    cubic = 0.044715
    square = pre_act * pre_act
    tanh = jnp.tanh(pre_act * (scale + scale * cubic * square))
    cdf = 0.5 + 0.5 * tanh
    slope = cdf + 0.5 * pre_act * (1.0 - tanh * tanh) * (scale + 3.0 * scale * cubic * square)
    return pre_act * cdf, slope


def chain_kernel(n_stage, n_data, n_model, own, acts, grad, g_up, g_down, mean, norm, wfull, slopes, gbuf, obuf, gathered, hid, slope, dz, sbuf, rbuf, part, slots,
                 wsend, wrecv, ysend, yrecv, gsend, grecv, csend, crecv, rsend, rrecv, nsend, nrecv):
    net = Net()
    z, y, s = net.z, net.y, net.s
    half, width = own.shape[2], own.shape[3]
    few = gbuf.shape[0]

    def z_copy(zs, mat, up, src):
        to = z + 1 if up else z - 1
        return net.send(src, wfull.at[zs, y, mat], wsend.at[int(up), zs, mat], wrecv.at[zs, mat], {'model': to})

    def y_copy(zs, mat, ys):
        return net.send(wfull.at[zs, ys, mat], wfull.at[zs, ys, mat], ysend.at[zs, mat], yrecv.at[zs, mat], {'data': net.y_other})

    def has_room(up):
        return (z < n_model - 1) if up else (z > 0)

    for mat in range(2):
        for up in (False, True):
            when_all([has_room(up)], lambda: z_copy(z, mat, up, own.at[mat, y]).start())
    for mat in range(2):
        for h in range(2):
            wfull[z, h, mat] = own[mat, h]

    up_own = own[0].reshape(2 * half, width)
    down_own = own[1].reshape(2 * half, width)

    def rows_at(k):
        return pl.ds(pl.multiple_of(k * few, few), few)

    def local_body(k, _):
        value, lean = gelu_parts(dot(acts[rows_at(k), :], own[0].reshape(2 * half, width)))
        hid[rows_at(k), :] = value.astype(BF16)
        slope[rows_at(k), :] = lean
        return 0

    lax.fori_loop(0, n_model, local_body, 0)

    for d in range(1, n_model):
        for mat in range(2):
            for side in range(2):
                zs, ok = side_of(z, n_model, d, side)
                up = side == 0
                def take():
                    z_copy(zs, mat, up, wfull.at[zs, y, mat]).wait_recv()
                    y_copy(zs, mat, y).start()
                when_all([ok], take)
                when_all([ok, has_room(up)], lambda: z_copy(zs, mat, up, wfull.at[zs, y, mat]).start())
    for d in range(1, n_model):
        for mat in range(2):
            for side in range(2):
                zs, ok = side_of(z, n_model, d, side)
                when_all([ok], lambda: y_copy(zs, mat, net.y_other).wait_recv())

    def pre_body(j, _):
        slopes[j] = gelu_parts(dot(acts[rows_at(z), :], wfull[j, :, 0].reshape(2 * half, width)))[1]
        return 0

    lax.fori_loop(0, n_model, pre_body, 0)

    g_in = net.send(obuf, gbuf, csend.at[0], crecv.at[0], {'stage': lax.max(s - 1, 0)})

    def g_copy(zs, up, src):
        to = z + 1 if up else z - 1
        return net.send(src, gathered.at[zs], gsend.at[int(up), zs], grecv.at[zs], {'model': to})

    @pl.when(s == n_stage - 1)
    def _():
        gbuf[...] = grad[rows_at(z), :]

    @pl.when(s < n_stage - 1)
    def _():
        g_in.wait_recv()
        for up in (False, True):
            when_all([has_room(up)], lambda: g_copy(z, up, gbuf).start())

    @pl.when(s > 0)
    def _():
        def back_body(j, total):
            grad_hid = dot(gbuf[...], wfull[j, :, 1].reshape(2 * half, width), CONTRACT_LAST)
            grad_pre = (grad_hid * slopes[j]).astype(BF16)
            return total + dot(grad_pre, wfull[j, :, 0].reshape(2 * half, width), CONTRACT_LAST)

        total = lax.fori_loop(0, n_model, back_body, jnp.zeros(gbuf.shape, F32))
        obuf[...] = (gbuf[...].astype(F32) + total).astype(BF16)
        g_in.start()

    @pl.when(s == n_stage - 1)
    def _():
        for k in range(n_model):
            gathered[k] = grad[k * few:(k + 1) * few, :]

    @pl.when(s < n_stage - 1)
    def _():
        gathered[z] = gbuf[...]
        for d in range(1, n_model):
            for side in range(2):
                zs, ok = side_of(z, n_model, d, side)
                up = side == 0
                when_all([ok], lambda: g_copy(zs, up, gathered.at[zs]).wait_recv())
                when_all([ok, has_room(up)], lambda: g_copy(zs, up, gathered.at[zs]).start())

    def dz_body(k, _):
        grad_hid = dot(gathered[k], own[1].reshape(2 * half, width), CONTRACT_LAST)
        dz[rows_at(k), :] = (grad_hid * slope[rows_at(k), :]).astype(BF16)
        return 0

    lax.fori_loop(0, n_model, dz_body, 0)
    grad_all = gathered[...].reshape(n_model * few, width)

    def half_grad(mat, ys):
        at = pl.ds(pl.multiple_of(ys * half, half), half)
        if mat == 0:
            return g_up[at, :] + dot(acts[:, at], dz[...], CONTRACT_FIRST)
        return g_down[at, :] + dot(hid[:, at], grad_all, CONTRACT_FIRST)

    def swap(mat):
        return net.send(sbuf.at[mat], rbuf.at[mat], rsend.at[mat], rrecv.at[mat], {'data': net.y_other})

    for mat in range(2):
        sbuf[mat] = half_grad(mat, net.y_other)
        swap(mat).start()
    for mat in range(2):
        mean[mat] = half_grad(mat, y)
    tile = jnp.zeros((8, 128), F32)
    for mat in range(2):
        swap(mat).wait_recv()
        both = (mean[mat] + rbuf[mat]) / n_data
        mean[mat] = both
        rowsum = jnp.sum((both * both).reshape(half // 8, 8, width), axis=0)
        for k in range(width // 128):
            tile = tile + rowsum[:, k * 128:(k + 1) * 128]

    count = n_stage * n_data * n_model
    me = (s * n_data + y) * n_model + z
    part[...] = tile

    def tell(k):
        other = lax.rem(me + k, count)
        to = {'model': lax.rem(other, n_model), 'data': lax.rem(other // n_model, n_data), 'stage': other // (n_model * n_data)}
        return net.send(part, slots.at[me], nsend.at[k], nrecv.at[me], to)

    def hear(k):
        other = lax.rem(me + k, count)
        return net.send(part, slots.at[other], nsend.at[k], nrecv.at[other], {'data': net.y_other})

    for k in range(1, count):
        tell(k).start()
    slots[me] = tile
    for k in range(1, count):
        hear(k).wait_recv()
    norm[...] = jnp.sum(slots[...], axis=0)

    for k in range(1, count):
        tell(k).wait_send()
    for mat in range(2):
        swap(mat).wait_send()
    for d in range(n_model):
        for side in range(2 if d else 1):
            zs, ok = side_of(z, n_model, d, side)
            for up in (False, True):
                if d and up != (side == 0):
                    continue
                for mat in range(2):
                    when_all([ok, has_room(up)], lambda: z_copy(zs, mat, up, wfull.at[zs, y, mat]).wait_send())
                when_all([ok, has_room(up), s < n_stage - 1], lambda: g_copy(zs, up, gathered.at[zs]).wait_send())
            if d:
                for mat in range(2):
                    when_all([ok], lambda: y_copy(zs, mat, y).wait_send())

    @pl.when(s > 0)
    def _():
        g_in.wait_send()


VMEM_SPEC = pl.BlockSpec(memory_space=pltpu.VMEM)
ANY_SPEC = pl.BlockSpec(memory_space=pl.ANY)
DMA = pltpu.SemaphoreType.DMA


def backward_all(own, acts, grad, g_up, g_down, n_stage, n_data, n_model):
    rows, width = acts.shape
    half = own.shape[2]
    few = rows // n_model
    count = n_stage * n_data * n_model
    return pl.pallas_call(
        functools.partial(chain_kernel, n_stage, n_data, n_model),
        out_shape=(jax.ShapeDtypeStruct((2, half, width), F32), jax.ShapeDtypeStruct((8, 128), F32)),
        in_specs=[VMEM_SPEC] * 5,
        out_specs=(VMEM_SPEC, VMEM_SPEC),
        scratch_shapes=[
            pltpu.VMEM((n_model, 2, 2, half, width), BF16),
            pltpu.VMEM((n_model, few, 2 * half), F32),
            pltpu.VMEM((few, width), BF16),
            pltpu.VMEM((few, width), BF16),
            pltpu.VMEM((n_model, few, width), BF16),
            pltpu.VMEM((rows, 2 * half), BF16),
            pltpu.VMEM((rows, 2 * half), F32),
            pltpu.VMEM((rows, 2 * half), BF16),
            pltpu.VMEM((2, half, width), F32),
            pltpu.VMEM((2, half, width), F32),
            pltpu.VMEM((8, 128), F32),
            pltpu.VMEM((count, 8, 128), F32),
            DMA((2, n_model, 2)), DMA((n_model, 2)), DMA((n_model, 2)), DMA((n_model, 2)),
            DMA((2, n_model)), DMA((n_model,)), DMA((1,)), DMA((1,)), DMA((2,)), DMA((2,)), DMA((count,)), DMA((count,)),
        ],
        compiler_params=pltpu.CompilerParams(has_side_effects=True, vmem_limit_bytes=60 * 1024 * 1024),
        name='backward',
    )(own, acts, grad, g_up, g_down)


def weights_kernel(n_model, own, new, zsend, xsend, ysend, csend, recv, local):
    net = Net()
    z, y, s = net.z, net.y, net.s
    c = lax.rem(s, 2)

    def slot(ss, zs, ys, mat):
        return new.at[ss, zs, ys, mat]

    def copy(src, ss, zs, ys, mat, sem, to):
        return net.send(src, slot(ss, zs, ys, mat), sem, recv.at[ss, zs, ys, mat], to)

    def go(kind, ss, zs, ys, mat, src=None):
        src = slot(ss, zs, ys, mat) if src is None else src
        if kind == 'up':
            return copy(src, ss, zs, ys, mat, zsend.at[1, zs, mat], {'model': z + 1})
        if kind == 'down':
            return copy(src, ss, zs, ys, mat, zsend.at[0, zs, mat], {'model': z - 1})
        if kind == 'x':
            return copy(src, ss, zs, ys, mat, xsend.at[zs, ys, mat], {'stage': net.s_across})
        if kind == 'y':
            return copy(src, ss, zs, ys, mat, ysend.at[ss // 2, zs, mat], {'data': net.y_other})
        return copy(src, ss, zs, ys, mat, csend.at[ss // 2, zs, ys, mat], {'stage': net.s_sibling})

    def arrive(ss, zs, ys, mat):
        go('c', ss, zs, ys, mat).wait_recv()

    def first(d, side, mat, act):
        zs, ok = side_of(z, n_model, d, side)
        src = own.at[mat] if d == 0 else None
        for kind in ('up', 'down'):
            if d and kind != ('up' if side == 0 else 'down'):
                continue
            room = (z < n_model - 1) if kind == 'up' else (z > 0)
            when_all([ok, room], lambda kind=kind: act(go(kind, s, zs, y, mat, src)))
        def rest():
            for kind in ('x', 'y', 'c'):
                act(go(kind, s, zs, y, mat, src))
        when_all([ok], rest)

    def beside(mat, zs):
        return (s, zs, net.y_other, mat) if mat == 0 else (net.s_across, zs, y, mat)

    def second(d, side, mat, act):
        zs, ok = side_of(z, n_model, d, side)
        ss, ys, kind = (net.s_across, y, 'y') if mat == 0 else (s, net.y_other, 'x')
        def rest():
            act(go(kind, ss, zs, ys, mat))
            act(go('c', ss, zs, ys, mat))
            act(go('c', *beside(mat, zs)))
        when_all([ok], rest)

    def third(d, side, mat, act):
        zs, ok = side_of(z, n_model, d, side)
        when_all([ok], lambda: act(go('c', net.s_across, zs, net.y_other, mat)))

    def start(copy):
        copy.start()

    def end(copy):
        copy.wait_send()

    def step(level, d):
        for side in range(2 if d else 1):
            for mat in range(2):
                zs, ok = side_of(z, n_model, d, side)
                if level == 0:
                    if d:
                        when_all([ok], lambda: arrive(s, zs, y, mat))
                    first(d, side, mat, start)
                elif level == 1:
                    ss, ys = (net.s_across, y) if mat == 0 else (s, net.y_other)
                    def both():
                        arrive(ss, zs, ys, mat)
                        arrive(*beside(mat, zs))
                    when_all([ok], both)
                    second(d, side, mat, start)
                else:
                    when_all([ok], lambda: arrive(net.s_across, zs, net.y_other, mat))
                    third(d, side, mat, start)

    mine = pltpu.make_async_copy(own, new.at[s, z, y], local.at[0])
    mine.start()
    for level, d in ((0, 0), (0, 1), (1, 0), (0, 2), (1, 1), (2, 0), (0, 3), (1, 2), (2, 1), (1, 3), (2, 2), (2, 3)):
        step(level, d)
    for ss in (net.s_sibling, lax.rem(net.s_sibling + 2, 4)):
        for zs in range(n_model):
            for ys in range(2):
                for mat in range(2):
                    arrive(ss, zs, ys, mat)
    for d in range(n_model):
        for side in range(2 if d else 1):
            for mat in range(2):
                first(d, side, mat, end)
                second(d, side, mat, end)
                third(d, side, mat, end)
    mine.wait()


def gather_weights(own, n_stage, n_model, n_data):
    n_mat, half, width = own.shape
    return pl.pallas_call(
        functools.partial(weights_kernel, n_model),
        out_shape=jax.ShapeDtypeStruct((n_stage, n_model, n_data, n_mat, half, width), BF16),
        in_specs=[VMEM_SPEC],
        out_specs=ANY_SPEC,
        scratch_shapes=[
            DMA((2, n_model, 2)), DMA((n_model, 2, 2)), DMA((2, n_model, 2)), DMA((2, n_model, 2, 2)),
            DMA((n_stage, n_model, n_data, n_mat)), DMA((1,)),
        ],
        compiler_params=pltpu.CompilerParams(has_side_effects=True),
        name='weights',
    )(own)


def out_kernel(n_model, pieces, own, out, zsend, xsend, csend, recv, local):
    net = Net()
    z, s = net.z, net.s
    last = len(pieces) - 1
    parts = [pl.ds(*piece) for piece in pieces]

    def slot(ss, zs, part):
        return out.at[ss * n_model + zs, parts[part]]

    def go(kind, ss, zs, part, src=None):
        src = slot(ss, zs, part) if src is None else src
        if kind == 'up':
            sem, to = zsend.at[1, ss // 2, zs, part], {'model': z + 1}
        elif kind == 'down':
            sem, to = zsend.at[0, ss // 2, zs, part], {'model': z - 1}
        elif kind == 'x':
            sem, to = xsend.at[zs, part], {'stage': net.s_across}
        else:
            sem, to = csend.at[ss // 2, zs, part], {'stage': net.s_sibling}
        return net.send(src, slot(ss, zs, part), sem, recv.at[ss, zs, part], to)

    def arrive(ss, zs, part):
        go('c', ss, zs, part).wait_recv()

    def source(ss, d, part):
        return own.at[parts[part]] if d == 0 and ss is s else None

    def pass_on(ss, d, side, part, act):
        zs, ok = side_of(z, n_model, d, side)
        src = source(ss, d, part)
        for kind in ('up', 'down'):
            if d and kind != ('up' if side == 0 else 'down'):
                continue
            room = (z < n_model - 1) if kind == 'up' else (z > 0)
            when_all([ok, room], lambda: act(go(kind, ss, zs, part, src)))
        def rest():
            if part < last:
                act(go('x', ss, zs, part, src))
            act(go('c', ss, zs, part, src))
        when_all([ok], rest)

    def across(d, side, part, act):
        zs, ok = side_of(z, n_model, d, side)
        when_all([ok], lambda: act(go('c', net.s_across, zs, part)))

    def start(copy):
        copy.start()

    def end(copy):
        copy.wait_send()

    def sides(d):
        return range(2 if d else 1)

    def take_across(d):
        for part in range(last):
            for side in sides(d):
                zs, ok = side_of(z, n_model, d, side)
                when_all([ok], lambda: arrive(net.s_across, zs, part))
                across(d, side, part, start)

    mine = pltpu.make_async_copy(own, out.at[s * n_model + z], local.at[0])
    mine.start()
    first = go('x', s, z, last, own.at[parts[last]])
    first.start()
    for part in range(last + 1):
        pass_on(s, 0, 0, part, start)
    arrive(net.s_across, z, last)
    pass_on(net.s_across, 0, 0, last, start)
    for d in range(1, n_model):
        for part in range(last):
            for side in sides(d):
                zs, ok = side_of(z, n_model, d, side)
                when_all([ok], lambda: arrive(s, zs, part))
                pass_on(s, d, side, part, start)
        for ss in (s, net.s_across):
            for side in sides(d):
                zs, ok = side_of(z, n_model, d, side)
                when_all([ok], lambda: arrive(ss, zs, last))
                pass_on(ss, d, side, last, start)
        take_across(d - 1)
    take_across(n_model - 1)
    for ss in (net.s_sibling, lax.rem(net.s_sibling + 2, 4)):
        for zs in range(n_model):
            for part in range(last + 1):
                arrive(ss, zs, part)
    first.wait_send()
    for d in range(n_model):
        for side in sides(d):
            for part in range(last + 1):
                pass_on(s, d, side, part, end)
            for part in range(last):
                across(d, side, part, end)
            pass_on(net.s_across, d, side, last, end)
    mine.wait()


def gather_out(own, n_stage, n_model):
    rows, width = own.shape
    unit = rows // 64
    pieces = ((0, 19 * unit), (19 * unit, 19 * unit), (38 * unit, 18 * unit), (56 * unit, 8 * unit))
    n_part = len(pieces)
    return pl.pallas_call(
        functools.partial(out_kernel, n_model, pieces),
        out_shape=jax.ShapeDtypeStruct((n_stage * n_model, rows, width), BF16),
        in_specs=[VMEM_SPEC],
        out_specs=ANY_SPEC,
        scratch_shapes=[
            DMA((2, 2, n_model, n_part)), DMA((n_model, n_part)), DMA((2, n_model, n_part)),
            DMA((n_stage, n_model, n_part)), DMA((1,)),
        ],
        compiler_params=pltpu.CompilerParams(has_side_effects=True, vmem_limit_bytes=4 * 1024 * 1024),
        name='gather_out',
    )(own)


def store_kernel(src, dst, sems):
    n_copy = sems.shape[0]
    step = src.shape[0] // n_copy
    copies = [pltpu.make_async_copy(src.at[pl.ds(k * step, step)], dst.at[pl.ds(k * step, step)], sems.at[k]) for k in range(n_copy)]
    for copy in copies:
        copy.start()
    for copy in copies:
        copy.wait()


def store_out(rows):
    return pl.pallas_call(
        store_kernel,
        out_shape=jax.ShapeDtypeStruct(rows.shape, rows.dtype),
        in_specs=[VMEM_SPEC],
        out_specs=ANY_SPEC,
        scratch_shapes=[DMA((8,))],
        compiler_params=pltpu.CompilerParams(vmem_limit_bytes=4 * 1024 * 1024),
        name='store_out',
    )(rows)


def mlp_kernel(rows_step, acts, up, down, out, cur, total):
    p, j = pl.program_id(0), pl.program_id(1)
    rows, width = cur.shape

    @pl.when((p == 0) & (j == 0))
    def _():
        cur[...] = acts[...]

    @pl.when(j == 0)
    def _():
        total[...] = jnp.zeros(total.shape, F32)

    up_w = up[0, 0, :, 0].reshape(width, width)
    down_w = down[0, 0, :, 0].reshape(width, width)
    n_step = rows // rows_step

    def at(r):
        return pl.ds(r * rows_step, rows_step)

    ahead = dot(cur[at(0), :], up_w)
    for r in range(n_step):
        pre = ahead
        if r + 1 < n_step:
            ahead = dot(cur[at(r + 1), :], up_w)
        total[at(r), :] += dot(gelu_parts(pre)[0].astype(BF16), down_w)

    @pl.when(j == pl.num_programs(1) - 1)
    def _():
        cur[...] = (cur[...].astype(F32) + total[...]).astype(BF16)

    @pl.when((p == pl.num_programs(0) - 1) & (j == pl.num_programs(1) - 1))
    def _():
        out[...] = cur[...]


def forward_rows(acts, new):
    n_stage, n_model, n_data, _, half, width = new.shape
    rows = acts.shape[0]
    def spec(mat):
        return pl.BlockSpec((1, 1, n_data, 1, half, width), lambda p, j: (p, j, 0, mat, 0, 0))
    whole = pl.BlockSpec((rows, width), lambda p, j: (0, 0))
    return pl.pallas_call(
        functools.partial(mlp_kernel, 256),
        out_shape=jax.ShapeDtypeStruct((rows, width), BF16),
        grid=(n_stage, n_model),
        in_specs=[whole, spec(0), spec(1)],
        out_specs=whole,
        scratch_shapes=[pltpu.VMEM((rows, width), BF16), pltpu.VMEM((rows, width), F32)],
        compiler_params=pltpu.CompilerParams(dimension_semantics=('arbitrary', 'arbitrary'), vmem_limit_bytes=40 * 1024 * 1024),
        cost_estimate=pl.CostEstimate(flops=4 * n_stage * rows * width * width * n_model, bytes_accessed=2 * new.size, transcendentals=n_stage * n_model * rows * width),
        name='forward',
    )(acts, new, new)


def solution(mesh):
    n_stage = mesh.shape['stage']
    n_data = mesh.shape['data']
    n_model = mesh.shape['model']
    swap = [(0, 1), (1, 0)]
    up_spec = P('stage', None, 'model')
    down_spec = P('stage', 'model', None)
    row_spec = P(None, 'data', None)
    in_specs = (up_spec, down_spec, up_spec, down_spec, up_spec, down_spec, P('data', 'stage', None, 'model'), P('data', 'stage', 'model', None), P('stage', 'data', None), P('data', None), row_spec, P(None), P(None))
    out_specs = (up_spec, down_spec, up_spec, down_spec, up_spec, down_spec, row_spec)

    def device_step(w_up, w_down, m_up, m_down, v_up, v_down, g_up, g_down, acts_last, grad_out, x_next, learn_rate, max_norm):
        stage_id = lax.axis_index('stage')
        model_id = lax.axis_index('model')
        data_id = lax.axis_index('data')
        acts_in = acts_last[0]
        w_up, w_down, m_up, m_down, v_up, v_down = (t[0] for t in (w_up, w_down, m_up, m_down, v_up, v_down))
        g_up, g_down = g_up[0, 0], g_down[0, 0]
        d_model, ff_local = w_up.shape
        half = d_model // n_data
        up_bf = w_up.astype(BF16)
        down_bf = w_down.astype(BF16)

        def half_of(arr, which):
            return lax.dynamic_slice_in_dim(arr, which * half, half, 0)

        own = jnp.stack([up_bf, down_bf]).reshape(2, n_data, half, d_model)
        mean, norm_tile = backward_all(own, acts_in, grad_out, g_up, g_down, n_stage, n_data, n_model)
        mean_up, mean_down = mean[0], mean[1]
        norm_sq = jnp.sum(norm_tile)
        clip = jnp.minimum(1.0, max_norm[0] / (jnp.sqrt(norm_sq) + NORM_EPS))
        step_rate = learn_rate[0]

        up_half = adamw_update(half_of(w_up, data_id), half_of(m_up, data_id), half_of(v_up, data_id), clip * mean_up, step_rate)[0]
        down_half = adamw_update(half_of(w_down, data_id), half_of(m_down, data_id), half_of(v_down, data_id), clip * mean_down, step_rate)[0]
        new = gather_weights(jnp.stack([up_half.astype(BF16), down_half.astype(BF16)]), n_stage, n_model, n_data)

        new, mean_up, mean_down = lax.optimization_barrier((new, mean_up, mean_down))
        other_up = lax.ppermute(mean_up, 'data', swap)
        other_down = lax.ppermute(mean_down, 'data', swap)

        def join(mine, other):
            first = jnp.where(data_id == 0, mine, other)
            second = jnp.where(data_id == 0, other, mine)
            return jnp.concatenate([first, second], axis=0)

        up_w, up_m, up_v = adamw_update(w_up, m_up, v_up, clip * join(mean_up, other_up), step_rate)
        down_w, down_m, down_v = adamw_update(w_down, m_down, v_down, clip * join(mean_down, other_down), step_rate)

        acts_cur = lax.dynamic_index_in_dim(x_next, stage_id * n_model + model_id, 0, keepdims=False)
        y_next = store_out(gather_out(forward_rows(acts_cur, new), n_stage, n_model))
        return (up_w[None], down_w[None], up_m[None], down_m[None], up_v[None], down_v[None], y_next)

    return jax.shard_map(device_step, mesh=mesh, in_specs=in_specs, out_specs=out_specs, check_vma=False)
```

```python
import functools

import jax
import jax.numpy as jnp
from jax import lax
from jax.experimental import pallas as pl
from jax.experimental.pallas import tpu as pltpu
from jax.sharding import PartitionSpec as P

ADAM_STEP = 10
BETA_ONE = 0.9
BETA_TWO = 0.95
ADAM_EPS = 1e-8
WEIGHT_DECAY = 0.1
NORM_EPS = 1e-6
CONTRACT_LAST = (((1,), (1,)), ((), ()))
CONTRACT_FIRST = (((0,), (0,)), ((), ()))
F32 = jnp.float32
BF16 = jnp.bfloat16


def adamw_update(weight, moment_one, moment_two, grad_step, step_rate):
    mom_new = BETA_ONE * moment_one + (1.0 - BETA_ONE) * grad_step
    sec_new = BETA_TWO * moment_two + (1.0 - BETA_TWO) * grad_step * grad_step
    one_corr = 1.0 - BETA_ONE ** ADAM_STEP
    two_corr = 1.0 - BETA_TWO ** ADAM_STEP
    direction = (mom_new / one_corr) / (jnp.sqrt(sec_new / two_corr) + ADAM_EPS)
    weight_new = weight - step_rate * (direction + WEIGHT_DECAY * weight)
    return weight_new, mom_new, sec_new


def dot(left, right, dims=None):
    if dims is None:
        return jnp.dot(left, right, preferred_element_type=F32)
    return lax.dot_general(left, right, dims, preferred_element_type=F32)


class Net:
    def __init__(self):
        self.z = lax.axis_index('model')
        self.y = lax.axis_index('data')
        self.s = lax.axis_index('stage')
        self.y_other = 1 - self.y
        self.s_across = lax.rem(self.s + 2, 4)
        self.s_sibling = self.s + 1 - 2 * lax.rem(self.s, 2)
        self.sends = []

    def send(self, src, dst, send_sem, recv_sem, to):
        return pltpu.make_async_remote_copy(src_ref=src, dst_ref=dst, send_sem=send_sem, recv_sem=recv_sem, device_id=to, device_id_type=pl.DeviceIdType.MESH)


def when_all(conds, body):
    cond = None
    for c in conds:
        if c is not None:
            cond = c if cond is None else cond & c
    if cond is None:
        body()
    else:
        pl.when(cond)(body)


def side_of(z, n_model, d, side):
    if d == 0:
        return z, None
    if side == 0:
        return lax.max(z - d, 0), z - d >= 0
    return lax.min(z + d, n_model - 1), z + d < n_model


def gelu_parts(pre_act):
    scale = 0.7978845608028654
    cubic = 0.044715
    square = pre_act * pre_act
    tanh = jnp.tanh(pre_act * (scale + scale * cubic * square))
    cdf = 0.5 + 0.5 * tanh
    slope = cdf + 0.5 * pre_act * (1.0 - tanh * tanh) * (scale + 3.0 * scale * cubic * square)
    return pre_act * cdf, slope


PER_MAT = 2


def chain_kernel(n_stage, n_data, n_model, own, acts_in, grad_in, g_up_in, g_down_in, mean, norm, acts, grad, g_up, g_down, wfull, slopes, gbuf, obuf, gathered, hid, slope, dz, sbuf, rbuf, part, slots,
                 wsend, wrecv, ysend, yrecv, gsend, grecv, dsend, csend, crecv, rsend, rrecv, nsend, nrecv, isem):
    net = Net()
    z, y, s = net.z, net.y, net.s
    half, width = own.shape[2], own.shape[3]
    few = gbuf.shape[0]

    n_piece = 2 * PER_MAT
    step = half // PER_MAT

    def full_piece(zs, ys, q):
        return wfull.at[zs, ys, q // PER_MAT, pl.ds(q % PER_MAT * step, step)]

    def z_copy(zs, q, up, src=None):
        to = z + 1 if up else z - 1
        src = full_piece(zs, y, q) if src is None else src
        return net.send(src, full_piece(zs, y, q), wsend.at[int(up), zs, q], wrecv.at[zs, q], {'model': to})

    def y_copy(zs, q, ys):
        return net.send(full_piece(zs, ys, q), full_piece(zs, ys, q), ysend.at[zs, q], yrecv.at[zs, q], {'data': net.y_other})

    def has_room(up):
        return (z < n_model - 1) if up else (z > 0)

    for q in range(n_piece):
        for up in (False, True):
            when_all([has_room(up)], lambda: z_copy(z, q, up, own.at[q // PER_MAT, y, pl.ds(q % PER_MAT * step, step)]).start())
    inputs = [pltpu.make_async_copy(src, dst, isem.at[k]) for k, (src, dst) in enumerate(((acts_in, acts), (grad_in, grad), (g_up_in, g_up), (g_down_in, g_down)))]
    for copy in inputs:
        copy.start()
    for mat in range(2):
        for h in range(2):
            wfull[z, h, mat] = own[mat, h]
    for copy in inputs:
        copy.wait()

    up_own = own[0].reshape(2 * half, width)
    down_own = own[1].reshape(2 * half, width)

    def rows_at(k):
        return pl.ds(pl.multiple_of(k * few, few), few)

    def local_body(k, _):
        value, lean = gelu_parts(dot(acts[rows_at(k), :], own[0].reshape(2 * half, width)))
        hid[rows_at(k), :] = value.astype(BF16)
        slope[rows_at(k), :] = lean
        return 0

    lax.fori_loop(0, n_model, local_body, 0)

    for d in range(1, n_model):
        for q in range(n_piece):
            for side in range(2):
                zs, ok = side_of(z, n_model, d, side)
                up = side == 0
                def take():
                    z_copy(zs, q, up).wait_recv()
                    y_copy(zs, q, y).start()
                when_all([ok], take)
                when_all([ok, has_room(up)], lambda: z_copy(zs, q, up).start())
    for d in range(1, n_model):
        for q in range(n_piece):
            for side in range(2):
                zs, ok = side_of(z, n_model, d, side)
                when_all([ok], lambda: y_copy(zs, q, net.y_other).wait_recv())

    def pre_body(j, _):
        slopes[j] = gelu_parts(dot(acts[rows_at(z), :], wfull[j, :, 0].reshape(2 * half, width)))[1]
        return 0

    lax.fori_loop(0, n_model, pre_body, 0)

    g_in = net.send(obuf, gbuf, csend.at[0], crecv.at[0], {'stage': lax.max(s - 1, 0)})

    def g_copy(zs, up, src):
        to = z + 1 if up else z - 1
        return net.send(src, gathered.at[zs], gsend.at[int(up), zs], grecv.at[zs], {'model': to})

    @pl.when(s == n_stage - 1)
    def _():
        gbuf[...] = grad[rows_at(z), :]

    def g_push(k):
        return net.send(gbuf, gathered.at[z], dsend.at[k], grecv.at[z], {'model': lax.rem(z + k, n_model)})

    def g_take(k):
        zs = lax.rem(z + k, n_model)
        return net.send(gbuf, gathered.at[zs], dsend.at[k], grecv.at[zs], {'data': net.y_other})

    @pl.when(s < n_stage - 1)
    def _():
        g_in.wait_recv()

    @pl.when((s > 0) & (s < n_stage - 1))
    def _():
        for k in (2, 1, 3):
            g_push(k).start()

    @pl.when(s == 0)
    def _():
        for up in (False, True):
            when_all([has_room(up)], lambda: g_copy(z, up, gbuf).start())

    @pl.when(s > 0)
    def _():
        def back_body(j, total):
            grad_hid = dot(gbuf[...], wfull[j, :, 1].reshape(2 * half, width), CONTRACT_LAST)
            grad_pre = (grad_hid * slopes[j]).astype(BF16)
            return total + dot(grad_pre, wfull[j, :, 0].reshape(2 * half, width), CONTRACT_LAST)

        total = lax.fori_loop(0, n_model, back_body, jnp.zeros(gbuf.shape, F32))
        obuf[...] = (gbuf[...].astype(F32) + total).astype(BF16)
        g_in.start()

    @pl.when(s == n_stage - 1)
    def _():
        for k in range(n_model):
            gathered[k] = grad[k * few:(k + 1) * few, :]

    @pl.when((s > 0) & (s < n_stage - 1))
    def _():
        gathered[z] = gbuf[...]
        for k in range(1, n_model):
            g_take(k).wait_recv()

    @pl.when(s == 0)
    def _():
        gathered[z] = gbuf[...]
        for d in range(1, n_model):
            for side in range(2):
                zs, ok = side_of(z, n_model, d, side)
                up = side == 0
                when_all([ok], lambda: g_copy(zs, up, gathered.at[zs]).wait_recv())
                when_all([ok, has_room(up)], lambda: g_copy(zs, up, gathered.at[zs]).start())

    def dz_body(k, _):
        grad_hid = dot(gathered[k], own[1].reshape(2 * half, width), CONTRACT_LAST)
        dz[rows_at(k), :] = (grad_hid * slope[rows_at(k), :]).astype(BF16)
        return 0

    lax.fori_loop(0, n_model, dz_body, 0)
    grad_all = gathered[...].reshape(n_model * few, width)

    def half_grad(mat, ys):
        at = pl.ds(pl.multiple_of(ys * half, half), half)
        if mat == 0:
            return g_up[at, :] + dot(acts[:, at], dz[...], CONTRACT_FIRST)
        return g_down[at, :] + dot(hid[:, at], grad_all, CONTRACT_FIRST)

    def swap(mat):
        return net.send(sbuf.at[mat], rbuf.at[mat], rsend.at[mat], rrecv.at[mat], {'data': net.y_other})

    for mat in range(2):
        sbuf[mat] = half_grad(mat, net.y_other)
        swap(mat).start()
    for mat in range(2):
        mean[mat] = half_grad(mat, y)
    tile = jnp.zeros((8, 128), F32)
    for mat in range(2):
        swap(mat).wait_recv()
        both = (mean[mat] + rbuf[mat]) / n_data
        mean[mat] = both
        rowsum = jnp.sum((both * both).reshape(half // 8, 8, width), axis=0)
        for k in range(width // 128):
            tile = tile + rowsum[:, k * 128:(k + 1) * 128]

    count = n_stage * n_data * n_model
    me = (s * n_data + y) * n_model + z
    part[...] = tile

    def tell(k):
        other = lax.rem(me + k, count)
        to = {'model': lax.rem(other, n_model), 'data': lax.rem(other // n_model, n_data), 'stage': other // (n_model * n_data)}
        return net.send(part, slots.at[me], nsend.at[k], nrecv.at[me], to)

    def hear(k):
        other = lax.rem(me + k, count)
        return net.send(part, slots.at[other], nsend.at[k], nrecv.at[other], {'data': net.y_other})

    for k in range(1, count):
        tell(k).start()
    slots[me] = tile
    for k in range(1, count):
        hear(k).wait_recv()
    norm[...] = jnp.sum(slots[...], axis=0)

    for k in range(1, count):
        tell(k).wait_send()
    for mat in range(2):
        swap(mat).wait_send()
    for d in range(n_model):
        for side in range(2 if d else 1):
            zs, ok = side_of(z, n_model, d, side)
            for up in (False, True):
                if d and up != (side == 0):
                    continue
                for q in range(n_piece):
                    when_all([ok, has_room(up)], lambda: z_copy(zs, q, up).wait_send())
                when_all([ok, has_room(up), s == 0], lambda: g_copy(zs, up, gathered.at[zs]).wait_send())
            if d:
                for q in range(n_piece):
                    when_all([ok], lambda: y_copy(zs, q, y).wait_send())

    @pl.when(s > 0)
    def _():
        g_in.wait_send()

    @pl.when((s > 0) & (s < n_stage - 1))
    def _():
        for k in range(1, n_model):
            g_push(k).wait_send()


VMEM_SPEC = pl.BlockSpec(memory_space=pltpu.VMEM)
ANY_SPEC = pl.BlockSpec(memory_space=pl.ANY)
DMA = pltpu.SemaphoreType.DMA


def backward_all(own, acts, grad, g_up, g_down, n_stage, n_data, n_model):
    rows, width = acts.shape
    half = own.shape[2]
    few = rows // n_model
    count = n_stage * n_data * n_model
    return pl.pallas_call(
        functools.partial(chain_kernel, n_stage, n_data, n_model),
        out_shape=(jax.ShapeDtypeStruct((2, half, width), F32), jax.ShapeDtypeStruct((8, 128), F32)),
        in_specs=[VMEM_SPEC] + [ANY_SPEC] * 4,
        out_specs=(VMEM_SPEC, VMEM_SPEC),
        scratch_shapes=[
            pltpu.VMEM((rows, width), BF16),
            pltpu.VMEM((rows, width), BF16),
            pltpu.VMEM((2 * half, width), F32),
            pltpu.VMEM((2 * half, width), F32),
            pltpu.VMEM((n_model, 2, 2, half, width), BF16),
            pltpu.VMEM((n_model, few, 2 * half), F32),
            pltpu.VMEM((few, width), BF16),
            pltpu.VMEM((few, width), BF16),
            pltpu.VMEM((n_model, few, width), BF16),
            pltpu.VMEM((rows, 2 * half), BF16),
            pltpu.VMEM((rows, 2 * half), F32),
            pltpu.VMEM((rows, 2 * half), BF16),
            pltpu.VMEM((2, half, width), F32),
            pltpu.VMEM((2, half, width), F32),
            pltpu.VMEM((8, 128), F32),
            pltpu.VMEM((count, 8, 128), F32),
            DMA((2, n_model, 2 * PER_MAT)), DMA((n_model, 2 * PER_MAT)), DMA((n_model, 2 * PER_MAT)), DMA((n_model, 2 * PER_MAT)),
            DMA((2, n_model)), DMA((n_model,)), DMA((n_model,)), DMA((1,)), DMA((1,)), DMA((2,)), DMA((2,)), DMA((count,)), DMA((count,)), DMA((4,)),
        ],
        compiler_params=pltpu.CompilerParams(has_side_effects=True, vmem_limit_bytes=60 * 1024 * 1024),
        name='backward',
    )(own, acts, grad, g_up, g_down)


def weights_kernel(n_model, own, new, zsend, xsend, ysend, csend, recv, local):
    net = Net()
    z, y, s = net.z, net.y, net.s
    c = lax.rem(s, 2)

    def slot(ss, zs, ys, mat):
        return new.at[ss, zs, ys, mat]

    def copy(src, ss, zs, ys, mat, sem, to):
        return net.send(src, slot(ss, zs, ys, mat), sem, recv.at[ss, zs, ys, mat], to)

    def go(kind, ss, zs, ys, mat, src=None):
        src = slot(ss, zs, ys, mat) if src is None else src
        if kind == 'up':
            return copy(src, ss, zs, ys, mat, zsend.at[1, zs, mat], {'model': z + 1})
        if kind == 'down':
            return copy(src, ss, zs, ys, mat, zsend.at[0, zs, mat], {'model': z - 1})
        if kind == 'x':
            return copy(src, ss, zs, ys, mat, xsend.at[zs, ys, mat], {'stage': net.s_across})
        if kind == 'y':
            return copy(src, ss, zs, ys, mat, ysend.at[ss // 2, zs, mat], {'data': net.y_other})
        return copy(src, ss, zs, ys, mat, csend.at[ss // 2, zs, ys, mat], {'stage': net.s_sibling})

    def arrive(ss, zs, ys, mat):
        go('c', ss, zs, ys, mat).wait_recv()

    def first(d, side, mat, act):
        zs, ok = side_of(z, n_model, d, side)
        src = own.at[mat] if d == 0 else None
        for kind in ('up', 'down'):
            if d and kind != ('up' if side == 0 else 'down'):
                continue
            room = (z < n_model - 1) if kind == 'up' else (z > 0)
            when_all([ok, room], lambda kind=kind: act(go(kind, s, zs, y, mat, src)))
        def rest():
            for kind in ('x', 'y', 'c'):
                act(go(kind, s, zs, y, mat, src))
        when_all([ok], rest)

    def beside(mat, zs):
        return (s, zs, net.y_other, mat) if mat == 0 else (net.s_across, zs, y, mat)

    def second(d, side, mat, act):
        zs, ok = side_of(z, n_model, d, side)
        ss, ys, kind = (net.s_across, y, 'y') if mat == 0 else (s, net.y_other, 'x')
        def rest():
            act(go(kind, ss, zs, ys, mat))
            act(go('c', ss, zs, ys, mat))
            act(go('c', *beside(mat, zs)))
        when_all([ok], rest)

    def third(d, side, mat, act):
        zs, ok = side_of(z, n_model, d, side)
        when_all([ok], lambda: act(go('c', net.s_across, zs, net.y_other, mat)))

    def start(copy):
        copy.start()

    def end(copy):
        copy.wait_send()

    def step(level, d):
        for side in range(2 if d else 1):
            for mat in range(2):
                zs, ok = side_of(z, n_model, d, side)
                if level == 0:
                    if d:
                        when_all([ok], lambda: arrive(s, zs, y, mat))
                    first(d, side, mat, start)
                elif level == 1:
                    ss, ys = (net.s_across, y) if mat == 0 else (s, net.y_other)
                    def both():
                        arrive(ss, zs, ys, mat)
                        arrive(*beside(mat, zs))
                    when_all([ok], both)
                    second(d, side, mat, start)
                else:
                    when_all([ok], lambda: arrive(net.s_across, zs, net.y_other, mat))
                    third(d, side, mat, start)

    mine = pltpu.make_async_copy(own, new.at[s, z, y], local.at[0])
    mine.start()
    for level, d in ((0, 0), (0, 1), (1, 0), (0, 2), (1, 1), (2, 0), (0, 3), (1, 2), (2, 1), (1, 3), (2, 2), (2, 3)):
        step(level, d)
    for ss in (net.s_sibling, lax.rem(net.s_sibling + 2, 4)):
        for zs in range(n_model):
            for ys in range(2):
                for mat in range(2):
                    arrive(ss, zs, ys, mat)
    for d in range(n_model):
        for side in range(2 if d else 1):
            for mat in range(2):
                first(d, side, mat, end)
                second(d, side, mat, end)
                third(d, side, mat, end)
    mine.wait()


def gather_weights(own, n_stage, n_model, n_data):
    n_mat, half, width = own.shape
    return pl.pallas_call(
        functools.partial(weights_kernel, n_model),
        out_shape=jax.ShapeDtypeStruct((n_stage, n_model, n_data, n_mat, half, width), BF16),
        in_specs=[VMEM_SPEC],
        out_specs=ANY_SPEC,
        scratch_shapes=[
            DMA((2, n_model, 2)), DMA((n_model, 2, 2)), DMA((2, n_model, 2)), DMA((2, n_model, 2, 2)),
            DMA((n_stage, n_model, n_data, n_mat)), DMA((1,)),
        ],
        compiler_params=pltpu.CompilerParams(has_side_effects=True),
        name='weights',
    )(own)


def out_kernel(n_model, pieces, groups, acts, new, out, own, total, wbuf, wsem, zsend, xsend, csend, recv, local):
    net = Net()
    z, s = net.z, net.s
    last = len(pieces) - 1
    parts = [pl.ds(*piece) for piece in pieces]

    def slot(ss, zs, part):
        return out.at[ss * n_model + zs, parts[part]]

    def go(kind, ss, zs, part, src=None):
        src = slot(ss, zs, part) if src is None else src
        if kind == 'up':
            sem, to = zsend.at[1, ss // 2, zs, part], {'model': z + 1}
        elif kind == 'down':
            sem, to = zsend.at[0, ss // 2, zs, part], {'model': z - 1}
        elif kind == 'x':
            sem, to = xsend.at[zs, part], {'stage': net.s_across}
        else:
            sem, to = csend.at[ss // 2, zs, part], {'stage': net.s_sibling}
        return net.send(src, slot(ss, zs, part), sem, recv.at[ss, zs, part], to)

    def arrive(ss, zs, part):
        go('c', ss, zs, part).wait_recv()

    def source(ss, d, part):
        return own.at[parts[part]] if d == 0 and ss is s else None

    def pass_on(ss, d, side, part, act):
        zs, ok = side_of(z, n_model, d, side)
        src = source(ss, d, part)
        for kind in ('up', 'down'):
            if d and kind != ('up' if side == 0 else 'down'):
                continue
            room = (z < n_model - 1) if kind == 'up' else (z > 0)
            when_all([ok, room], lambda: act(go(kind, ss, zs, part, src)))
        def rest():
            if part < last:
                act(go('x', ss, zs, part, src))
            act(go('c', ss, zs, part, src))
        when_all([ok], rest)

    def across(d, side, part, act):
        zs, ok = side_of(z, n_model, d, side)
        when_all([ok], lambda: act(go('c', net.s_across, zs, part)))

    def start(copy):
        copy.start()

    def end(copy):
        copy.wait_send()

    def sides(d):
        return range(2 if d else 1)

    def take_across(d):
        for part in range(last):
            for side in sides(d):
                zs, ok = side_of(z, n_model, d, side)
                when_all([ok], lambda: arrive(net.s_across, zs, part))
                across(d, side, part, start)

    n_block = new.shape[0] * n_model
    width = own.shape[1]
    few = 128

    def fetch(t):
        slot_of = lax.rem(t, 2)
        return pltpu.make_async_copy(new.at[lax.rem(t, n_block) // n_model, lax.rem(t, n_model)], wbuf.at[slot_of], wsem.at[slot_of])

    own[...] = acts[...]
    fetch(0).start()
    for n, (base, count, ready) in enumerate(groups):
        def block(t, _, base=base, count=count):
            fetch(t).wait()

            @pl.when(t + 1 < n_block * len(groups))
            def _():
                fetch(t + 1).start()

            turn = lax.rem(t, n_model)

            @pl.when(turn == 0)
            def _():
                total[...] = jnp.zeros(total.shape, F32)

            held = wbuf.at[lax.rem(t, 2)]
            up_w = held[:, 0].reshape(width, width)
            down_w = held[:, 1].reshape(width, width)
            ahead = dot(own[base:base + few, :], up_w)
            for r in range(count // few):
                pre = ahead
                if (r + 1) * few < count:
                    ahead = dot(own[base + (r + 1) * few:base + (r + 2) * few, :], up_w)
                total[r * few:(r + 1) * few, :] += dot(gelu_parts(pre)[0].astype(BF16), down_w)

            @pl.when(turn == n_model - 1)
            def _():
                own[base:base + count, :] = (own[base:base + count, :].astype(F32) + total[:count, :]).astype(BF16)

            return 0

        lax.fori_loop(n * n_block, (n + 1) * n_block, block, 0)
        if last in ready:
            first = go('x', s, z, last, own.at[parts[last]])
            first.start()
        for part in ready:
            pass_on(s, 0, 0, part, start)
    mine = pltpu.make_async_copy(own, out.at[s * n_model + z], local.at[0])
    mine.start()
    arrive(net.s_across, z, last)
    pass_on(net.s_across, 0, 0, last, start)
    for d in range(1, n_model):
        for part in range(last):
            for side in sides(d):
                zs, ok = side_of(z, n_model, d, side)
                when_all([ok], lambda: arrive(s, zs, part))
                pass_on(s, d, side, part, start)
        for ss in (s, net.s_across):
            for side in sides(d):
                zs, ok = side_of(z, n_model, d, side)
                when_all([ok], lambda: arrive(ss, zs, last))
                pass_on(ss, d, side, last, start)
        take_across(d - 1)
    take_across(n_model - 1)
    for ss in (net.s_sibling, lax.rem(net.s_sibling + 2, 4)):
        for zs in range(n_model):
            for part in range(last + 1):
                arrive(ss, zs, part)
    first.wait_send()
    for d in range(n_model):
        for side in sides(d):
            for part in range(last + 1):
                pass_on(s, d, side, part, end)
            for part in range(last):
                across(d, side, part, end)
            pass_on(net.s_across, d, side, last, end)
    mine.wait()


def forward_out(acts, new):
    n_stage, n_model, n_data, n_mat, half, width = new.shape
    rows = acts.shape[0]
    unit = rows // 64
    pieces = ((8 * unit, 12 * unit), (20 * unit, 12 * unit), (32 * unit, 16 * unit), (48 * unit, 16 * unit), (0, 8 * unit))
    groups = ((0, rows // 2, (4, 0, 1)), (rows // 2, rows // 2, (2, 3)))
    n_part = len(pieces)
    return pl.pallas_call(
        functools.partial(out_kernel, n_model, pieces, groups),
        out_shape=jax.ShapeDtypeStruct((n_stage * n_model, rows, width), BF16),
        in_specs=[VMEM_SPEC, ANY_SPEC],
        out_specs=ANY_SPEC,
        scratch_shapes=[
            pltpu.VMEM((rows, width), BF16), pltpu.VMEM((rows // 2, width), F32), pltpu.VMEM((2, n_data, n_mat, half, width), BF16), DMA((2,)),
            DMA((2, 2, n_model, n_part)), DMA((n_model, n_part)), DMA((2, n_model, n_part)),
            DMA((n_stage, n_model, n_part)), DMA((1,)),
        ],
        compiler_params=pltpu.CompilerParams(has_side_effects=True, vmem_limit_bytes=20 * 1024 * 1024),
        name='forward_out',
    )(acts, new)


def store_kernel(src, dst, sems):
    n_copy = sems.shape[0]
    step = src.shape[0] // n_copy
    copies = [pltpu.make_async_copy(src.at[pl.ds(k * step, step)], dst.at[pl.ds(k * step, step)], sems.at[k]) for k in range(n_copy)]
    for copy in copies:
        copy.start()
    for copy in copies:
        copy.wait()


def store_out(rows):
    return pl.pallas_call(
        store_kernel,
        out_shape=jax.ShapeDtypeStruct(rows.shape, rows.dtype),
        in_specs=[VMEM_SPEC],
        out_specs=ANY_SPEC,
        scratch_shapes=[DMA((8,))],
        compiler_params=pltpu.CompilerParams(vmem_limit_bytes=4 * 1024 * 1024),
        name='store_out',
    )(rows)


def solution(mesh):
    n_stage = mesh.shape['stage']
    n_data = mesh.shape['data']
    n_model = mesh.shape['model']
    swap = [(0, 1), (1, 0)]
    up_spec = P('stage', None, 'model')
    down_spec = P('stage', 'model', None)
    row_spec = P(None, 'data', None)
    in_specs = (up_spec, down_spec, up_spec, down_spec, up_spec, down_spec, P('data', 'stage', None, 'model'), P('data', 'stage', 'model', None), P('stage', 'data', None), P('data', None), row_spec, P(None), P(None))
    out_specs = (up_spec, down_spec, up_spec, down_spec, up_spec, down_spec, row_spec)

    def device_step(w_up, w_down, m_up, m_down, v_up, v_down, g_up, g_down, acts_last, grad_out, x_next, learn_rate, max_norm):
        stage_id = lax.axis_index('stage')
        model_id = lax.axis_index('model')
        data_id = lax.axis_index('data')
        acts_in = acts_last[0]
        w_up, w_down, m_up, m_down, v_up, v_down = (t[0] for t in (w_up, w_down, m_up, m_down, v_up, v_down))
        g_up, g_down = g_up[0, 0], g_down[0, 0]
        d_model, ff_local = w_up.shape
        half = d_model // n_data
        up_bf = w_up.astype(BF16)
        down_bf = w_down.astype(BF16)

        def half_of(arr, which):
            return lax.dynamic_slice_in_dim(arr, which * half, half, 0)

        own = jnp.stack([up_bf, down_bf]).reshape(2, n_data, half, d_model)
        mean, norm_tile = backward_all(own, acts_in, grad_out, g_up, g_down, n_stage, n_data, n_model)
        mean_up, mean_down = mean[0], mean[1]
        norm_sq = jnp.sum(norm_tile)
        clip = jnp.minimum(1.0, max_norm[0] / (jnp.sqrt(norm_sq) + NORM_EPS))
        step_rate = learn_rate[0]

        up_half = adamw_update(half_of(w_up, data_id), half_of(m_up, data_id), half_of(v_up, data_id), clip * mean_up, step_rate)[0]
        down_half = adamw_update(half_of(w_down, data_id), half_of(m_down, data_id), half_of(v_down, data_id), clip * mean_down, step_rate)[0]
        new = gather_weights(jnp.stack([up_half.astype(BF16), down_half.astype(BF16)]), n_stage, n_model, n_data)

        new, mean_up, mean_down = lax.optimization_barrier((new, mean_up, mean_down))
        other_up = lax.ppermute(mean_up, 'data', swap)
        other_down = lax.ppermute(mean_down, 'data', swap)

        def join(mine, other):
            first = jnp.where(data_id == 0, mine, other)
            second = jnp.where(data_id == 0, other, mine)
            return jnp.concatenate([first, second], axis=0)

        up_w, up_m, up_v = adamw_update(w_up, m_up, v_up, clip * join(mean_up, other_up), step_rate)
        down_w, down_m, down_v = adamw_update(w_down, m_down, v_down, clip * join(mean_down, other_down), step_rate)

        acts_cur = lax.dynamic_index_in_dim(x_next, stage_id * n_model + model_id, 0, keepdims=False)
        y_next = store_out(forward_out(acts_cur, new))
        return (up_w[None], down_w[None], up_m[None], down_m[None], up_v[None], down_v[None], y_next)

    return jax.shard_map(device_step, mesh=mesh, in_specs=in_specs, out_specs=out_specs, check_vma=False)
```

```python
import functools

import jax
import jax.numpy as jnp
from jax import lax
from jax.experimental import pallas as pl
from jax.experimental.pallas import tpu as pltpu
from jax.sharding import PartitionSpec as P

ADAM_STEP = 10
BETA_ONE = 0.9
BETA_TWO = 0.95
ADAM_EPS = 1e-8
WEIGHT_DECAY = 0.1
NORM_EPS = 1e-6
CONTRACT_LAST = (((1,), (1,)), ((), ()))
CONTRACT_FIRST = (((0,), (0,)), ((), ()))
F32 = jnp.float32
BF16 = jnp.bfloat16


def adamw_update(weight, moment_one, moment_two, grad_step, step_rate):
    mom_new = BETA_ONE * moment_one + (1.0 - BETA_ONE) * grad_step
    sec_new = BETA_TWO * moment_two + (1.0 - BETA_TWO) * grad_step * grad_step
    one_corr = 1.0 - BETA_ONE ** ADAM_STEP
    two_corr = 1.0 - BETA_TWO ** ADAM_STEP
    direction = (mom_new / one_corr) / (jnp.sqrt(sec_new / two_corr) + ADAM_EPS)
    weight_new = weight - step_rate * (direction + WEIGHT_DECAY * weight)
    return weight_new, mom_new, sec_new


def dot(left, right, dims=None):
    if dims is None:
        return jnp.dot(left, right, preferred_element_type=F32)
    return lax.dot_general(left, right, dims, preferred_element_type=F32)


class Net:
    def __init__(self):
        self.z = lax.axis_index('model')
        self.y = lax.axis_index('data')
        self.s = lax.axis_index('stage')
        self.y_other = 1 - self.y
        self.s_across = lax.rem(self.s + 2, 4)
        self.s_sibling = self.s + 1 - 2 * lax.rem(self.s, 2)
        self.sends = []

    def send(self, src, dst, send_sem, recv_sem, to):
        return pltpu.make_async_remote_copy(src_ref=src, dst_ref=dst, send_sem=send_sem, recv_sem=recv_sem, device_id=to, device_id_type=pl.DeviceIdType.MESH)


def when_all(conds, body):
    cond = None
    for c in conds:
        if c is not None:
            cond = c if cond is None else cond & c
    if cond is None:
        body()
    else:
        pl.when(cond)(body)


def side_of(z, n_model, d, side):
    if d == 0:
        return z, None
    if side == 0:
        return lax.max(z - d, 0), z - d >= 0
    return lax.min(z + d, n_model - 1), z + d < n_model


def gelu_parts(pre_act):
    scale = 0.7978845608028654
    cubic = 0.044715
    square = pre_act * pre_act
    tanh = jnp.tanh(pre_act * (scale + scale * cubic * square))
    cdf = 0.5 + 0.5 * tanh
    slope = cdf + 0.5 * pre_act * (1.0 - tanh * tanh) * (scale + 3.0 * scale * cubic * square)
    return pre_act * cdf, slope


PER_MAT = 2


def chain_kernel(n_stage, n_data, n_model, own, acts_in, grad_in, g_up_in, g_down_in, mean, norm, acts, grad, g_up, g_down, wfull, slopes, gbuf, obuf, gathered, hid, slope, dz, sbuf, rbuf, part, slots,
                 wsend, wrecv, ysend, yrecv, gsend, grecv, dsend, csend, crecv, rsend, rrecv, nsend, nrecv, isem):
    net = Net()
    z, y, s = net.z, net.y, net.s
    half, width = own.shape[2], own.shape[3]
    few = gbuf.shape[0]

    n_piece = 2 * PER_MAT
    step = half // PER_MAT

    def full_piece(zs, ys, q):
        return wfull.at[zs, ys, q // PER_MAT, pl.ds(q % PER_MAT * step, step)]

    def z_copy(zs, q, up, src=None):
        to = z + 1 if up else z - 1
        src = full_piece(zs, y, q) if src is None else src
        return net.send(src, full_piece(zs, y, q), wsend.at[int(up), zs, q], wrecv.at[zs, q], {'model': to})

    def y_copy(zs, q, ys):
        return net.send(full_piece(zs, ys, q), full_piece(zs, ys, q), ysend.at[zs, q], yrecv.at[zs, q], {'data': net.y_other})

    def has_room(up):
        return (z < n_model - 1) if up else (z > 0)

    for q in range(n_piece):
        for up in (False, True):
            when_all([has_room(up)], lambda: z_copy(z, q, up, own.at[q // PER_MAT, y, pl.ds(q % PER_MAT * step, step)]).start())
    inputs = [pltpu.make_async_copy(src, dst, isem.at[k]) for k, (src, dst) in enumerate(((acts_in, acts), (grad_in, grad), (g_up_in, g_up), (g_down_in, g_down)))]
    for copy in inputs:
        copy.start()
    for mat in range(2):
        for h in range(2):
            wfull[z, h, mat] = own[mat, h]
    for copy in inputs:
        copy.wait()

    up_own = own[0].reshape(2 * half, width)
    down_own = own[1].reshape(2 * half, width)

    def rows_at(k):
        return pl.ds(pl.multiple_of(k * few, few), few)

    def local_body(k, _):
        value, lean = gelu_parts(dot(acts[rows_at(k), :], own[0].reshape(2 * half, width)))
        hid[rows_at(k), :] = value.astype(BF16)
        slope[rows_at(k), :] = lean
        return 0

    lax.fori_loop(0, n_model, local_body, 0)

    for d in range(1, n_model):
        for q in range(n_piece):
            for side in range(2):
                zs, ok = side_of(z, n_model, d, side)
                up = side == 0
                def take():
                    z_copy(zs, q, up).wait_recv()
                    y_copy(zs, q, y).start()
                when_all([ok], take)
                when_all([ok, has_room(up)], lambda: z_copy(zs, q, up).start())
    for d in range(1, n_model):
        for q in range(n_piece):
            for side in range(2):
                zs, ok = side_of(z, n_model, d, side)
                when_all([ok], lambda: y_copy(zs, q, net.y_other).wait_recv())

    def pre_body(j, _):
        slopes[j] = gelu_parts(dot(acts[rows_at(z), :], wfull[j, :, 0].reshape(2 * half, width)))[1]
        return 0

    lax.fori_loop(0, n_model, pre_body, 0)

    g_in = net.send(obuf, gbuf, csend.at[0], crecv.at[0], {'stage': lax.max(s - 1, 0)})

    def g_copy(zs, up, src):
        to = z + 1 if up else z - 1
        return net.send(src, gathered.at[zs], gsend.at[int(up), zs], grecv.at[zs], {'model': to})

    @pl.when(s == n_stage - 1)
    def _():
        gbuf[...] = grad[rows_at(z), :]

    def g_push(k):
        return net.send(gbuf, gathered.at[z], dsend.at[k], grecv.at[z], {'model': lax.rem(z + k, n_model)})

    def g_take(k):
        zs = lax.rem(z + k, n_model)
        return net.send(gbuf, gathered.at[zs], dsend.at[k], grecv.at[zs], {'data': net.y_other})

    @pl.when(s < n_stage - 1)
    def _():
        g_in.wait_recv()

    @pl.when((s > 0) & (s < n_stage - 1))
    def _():
        for k in (2, 1, 3):
            g_push(k).start()

    @pl.when(s == 0)
    def _():
        for up in (False, True):
            when_all([has_room(up)], lambda: g_copy(z, up, gbuf).start())

    @pl.when(s > 0)
    def _():
        def back_body(j, total):
            grad_hid = dot(gbuf[...], wfull[j, :, 1].reshape(2 * half, width), CONTRACT_LAST)
            grad_pre = (grad_hid * slopes[j]).astype(BF16)
            return total + dot(grad_pre, wfull[j, :, 0].reshape(2 * half, width), CONTRACT_LAST)

        total = lax.fori_loop(0, n_model, back_body, jnp.zeros(gbuf.shape, F32))
        obuf[...] = (gbuf[...].astype(F32) + total).astype(BF16)
        g_in.start()

    @pl.when(s == n_stage - 1)
    def _():
        for k in range(n_model):
            gathered[k] = grad[k * few:(k + 1) * few, :]

    @pl.when((s > 0) & (s < n_stage - 1))
    def _():
        gathered[z] = gbuf[...]
        for k in range(1, n_model):
            g_take(k).wait_recv()

    @pl.when(s == 0)
    def _():
        gathered[z] = gbuf[...]
        for d in range(1, n_model):
            for side in range(2):
                zs, ok = side_of(z, n_model, d, side)
                up = side == 0
                when_all([ok], lambda: g_copy(zs, up, gathered.at[zs]).wait_recv())
                when_all([ok, has_room(up)], lambda: g_copy(zs, up, gathered.at[zs]).start())

    def dz_body(k, _):
        grad_hid = dot(gathered[k], own[1].reshape(2 * half, width), CONTRACT_LAST)
        dz[rows_at(k), :] = (grad_hid * slope[rows_at(k), :]).astype(BF16)
        return 0

    lax.fori_loop(0, n_model, dz_body, 0)
    grad_all = gathered[...].reshape(n_model * few, width)

    def half_grad(mat, ys):
        at = pl.ds(pl.multiple_of(ys * half, half), half)
        if mat == 0:
            return g_up[at, :] + dot(acts[:, at], dz[...], CONTRACT_FIRST)
        return g_down[at, :] + dot(hid[:, at], grad_all, CONTRACT_FIRST)

    def swap(mat):
        return net.send(sbuf.at[mat], rbuf.at[mat], rsend.at[mat], rrecv.at[mat], {'data': net.y_other})

    for mat in range(2):
        sbuf[mat] = half_grad(mat, net.y_other)
        swap(mat).start()
    for mat in range(2):
        mean[mat] = half_grad(mat, y)
    tile = jnp.zeros((8, 128), F32)
    for mat in range(2):
        swap(mat).wait_recv()
        both = (mean[mat] + rbuf[mat]) / n_data
        mean[mat] = both
        rowsum = jnp.sum((both * both).reshape(half // 8, 8, width), axis=0)
        for k in range(width // 128):
            tile = tile + rowsum[:, k * 128:(k + 1) * 128]

    count = n_stage * n_data * n_model
    me = (s * n_data + y) * n_model + z
    part[...] = tile

    def tell(k):
        other = lax.rem(me + k, count)
        to = {'model': lax.rem(other, n_model), 'data': lax.rem(other // n_model, n_data), 'stage': other // (n_model * n_data)}
        return net.send(part, slots.at[me], nsend.at[k], nrecv.at[me], to)

    def hear(k):
        other = lax.rem(me + k, count)
        return net.send(part, slots.at[other], nsend.at[k], nrecv.at[other], {'data': net.y_other})

    for k in range(1, count):
        tell(k).start()
    slots[me] = tile
    for k in range(1, count):
        hear(k).wait_recv()
    norm[...] = jnp.sum(slots[...], axis=0)

    for k in range(1, count):
        tell(k).wait_send()
    for mat in range(2):
        swap(mat).wait_send()
    for d in range(n_model):
        for side in range(2 if d else 1):
            zs, ok = side_of(z, n_model, d, side)
            for up in (False, True):
                if d and up != (side == 0):
                    continue
                for q in range(n_piece):
                    when_all([ok, has_room(up)], lambda: z_copy(zs, q, up).wait_send())
                when_all([ok, has_room(up), s == 0], lambda: g_copy(zs, up, gathered.at[zs]).wait_send())
            if d:
                for q in range(n_piece):
                    when_all([ok], lambda: y_copy(zs, q, y).wait_send())

    @pl.when(s > 0)
    def _():
        g_in.wait_send()

    @pl.when((s > 0) & (s < n_stage - 1))
    def _():
        for k in range(1, n_model):
            g_push(k).wait_send()


VMEM_SPEC = pl.BlockSpec(memory_space=pltpu.VMEM)
ANY_SPEC = pl.BlockSpec(memory_space=pl.ANY)
DMA = pltpu.SemaphoreType.DMA


def backward_all(own, acts, grad, g_up, g_down, n_stage, n_data, n_model):
    rows, width = acts.shape
    half = own.shape[2]
    few = rows // n_model
    count = n_stage * n_data * n_model
    return pl.pallas_call(
        functools.partial(chain_kernel, n_stage, n_data, n_model),
        out_shape=(jax.ShapeDtypeStruct((2, half, width), F32), jax.ShapeDtypeStruct((8, 128), F32)),
        in_specs=[VMEM_SPEC] + [ANY_SPEC] * 4,
        out_specs=(VMEM_SPEC, VMEM_SPEC),
        scratch_shapes=[
            pltpu.VMEM((rows, width), BF16),
            pltpu.VMEM((rows, width), BF16),
            pltpu.VMEM((2 * half, width), F32),
            pltpu.VMEM((2 * half, width), F32),
            pltpu.VMEM((n_model, 2, 2, half, width), BF16),
            pltpu.VMEM((n_model, few, 2 * half), F32),
            pltpu.VMEM((few, width), BF16),
            pltpu.VMEM((few, width), BF16),
            pltpu.VMEM((n_model, few, width), BF16),
            pltpu.VMEM((rows, 2 * half), BF16),
            pltpu.VMEM((rows, 2 * half), F32),
            pltpu.VMEM((rows, 2 * half), BF16),
            pltpu.VMEM((2, half, width), F32),
            pltpu.VMEM((2, half, width), F32),
            pltpu.VMEM((8, 128), F32),
            pltpu.VMEM((count, 8, 128), F32),
            DMA((2, n_model, 2 * PER_MAT)), DMA((n_model, 2 * PER_MAT)), DMA((n_model, 2 * PER_MAT)), DMA((n_model, 2 * PER_MAT)),
            DMA((2, n_model)), DMA((n_model,)), DMA((n_model,)), DMA((1,)), DMA((1,)), DMA((2,)), DMA((2,)), DMA((count,)), DMA((count,)), DMA((4,)),
        ],
        compiler_params=pltpu.CompilerParams(has_side_effects=True, vmem_limit_bytes=60 * 1024 * 1024),
        name='backward',
    )(own, acts, grad, g_up, g_down)


def weights_kernel(n_model, own, new, zsend, xsend, ysend, csend, recv, local):
    net = Net()
    z, y, s = net.z, net.y, net.s
    c = lax.rem(s, 2)

    def slot(ss, zs, ys, mat):
        return new.at[ss, zs, ys, mat]

    def copy(src, ss, zs, ys, mat, sem, to):
        return net.send(src, slot(ss, zs, ys, mat), sem, recv.at[ss, zs, ys, mat], to)

    def go(kind, ss, zs, ys, mat, src=None):
        src = slot(ss, zs, ys, mat) if src is None else src
        if kind == 'up':
            return copy(src, ss, zs, ys, mat, zsend.at[1, zs, mat], {'model': z + 1})
        if kind == 'down':
            return copy(src, ss, zs, ys, mat, zsend.at[0, zs, mat], {'model': z - 1})
        if kind == 'x':
            return copy(src, ss, zs, ys, mat, xsend.at[zs, ys, mat], {'stage': net.s_across})
        if kind == 'y':
            return copy(src, ss, zs, ys, mat, ysend.at[ss // 2, zs, mat], {'data': net.y_other})
        return copy(src, ss, zs, ys, mat, csend.at[ss // 2, zs, ys, mat], {'stage': net.s_sibling})

    def arrive(ss, zs, ys, mat):
        go('c', ss, zs, ys, mat).wait_recv()

    def first(d, side, mat, act):
        zs, ok = side_of(z, n_model, d, side)
        src = own.at[mat] if d == 0 else None
        for kind in ('up', 'down'):
            if d and kind != ('up' if side == 0 else 'down'):
                continue
            room = (z < n_model - 1) if kind == 'up' else (z > 0)
            when_all([ok, room], lambda kind=kind: act(go(kind, s, zs, y, mat, src)))
        def rest():
            for kind in ('x', 'y', 'c'):
                act(go(kind, s, zs, y, mat, src))
        when_all([ok], rest)

    def beside(mat, zs):
        return (s, zs, net.y_other, mat) if mat == 0 else (net.s_across, zs, y, mat)

    def second(d, side, mat, act):
        zs, ok = side_of(z, n_model, d, side)
        ss, ys, kind = (net.s_across, y, 'y') if mat == 0 else (s, net.y_other, 'x')
        def rest():
            act(go(kind, ss, zs, ys, mat))
            act(go('c', ss, zs, ys, mat))
            act(go('c', *beside(mat, zs)))
        when_all([ok], rest)

    def third(d, side, mat, act):
        zs, ok = side_of(z, n_model, d, side)
        when_all([ok], lambda: act(go('c', net.s_across, zs, net.y_other, mat)))

    def start(copy):
        copy.start()

    def end(copy):
        copy.wait_send()

    def step(level, d):
        for side in range(2 if d else 1):
            for mat in range(2):
                zs, ok = side_of(z, n_model, d, side)
                if level == 0:
                    if d:
                        when_all([ok], lambda: arrive(s, zs, y, mat))
                    first(d, side, mat, start)
                elif level == 1:
                    ss, ys = (net.s_across, y) if mat == 0 else (s, net.y_other)
                    def both():
                        arrive(ss, zs, ys, mat)
                        arrive(*beside(mat, zs))
                    when_all([ok], both)
                    second(d, side, mat, start)
                else:
                    when_all([ok], lambda: arrive(net.s_across, zs, net.y_other, mat))
                    third(d, side, mat, start)

    mine = pltpu.make_async_copy(own, new.at[s, z, y], local.at[0])
    mine.start()
    for level, d in ((0, 0), (0, 1), (1, 0), (0, 2), (1, 1), (2, 0), (0, 3), (1, 2), (2, 1), (1, 3), (2, 2), (2, 3)):
        step(level, d)
    for ss in (net.s_sibling, lax.rem(net.s_sibling + 2, 4)):
        for zs in range(n_model):
            for ys in range(2):
                for mat in range(2):
                    arrive(ss, zs, ys, mat)
    for d in range(n_model):
        for side in range(2 if d else 1):
            for mat in range(2):
                first(d, side, mat, end)
                second(d, side, mat, end)
                third(d, side, mat, end)
    mine.wait()


def gather_weights(own, n_stage, n_model, n_data):
    n_mat, half, width = own.shape
    return pl.pallas_call(
        functools.partial(weights_kernel, n_model),
        out_shape=jax.ShapeDtypeStruct((n_stage, n_model, n_data, n_mat, half, width), BF16),
        in_specs=[VMEM_SPEC],
        out_specs=ANY_SPEC,
        scratch_shapes=[
            DMA((2, n_model, 2)), DMA((n_model, 2, 2)), DMA((2, n_model, 2)), DMA((2, n_model, 2, 2)),
            DMA((n_stage, n_model, n_data, n_mat)), DMA((1,)),
        ],
        compiler_params=pltpu.CompilerParams(has_side_effects=True),
        name='weights',
    )(own)


def out_kernel(n_model, pieces, groups, acts, new, out, own, total, wbuf, wsem, zsend, xsend, csend, recv, local):
    net = Net()
    z, s = net.z, net.s
    last = len(pieces) - 1
    parts = [pl.ds(*piece) for piece in pieces]

    def slot(ss, zs, part):
        return out.at[ss * n_model + zs, parts[part]]

    def go(kind, ss, zs, part, src=None):
        src = slot(ss, zs, part) if src is None else src
        if kind == 'up':
            sem, to = zsend.at[1, ss // 2, zs, part], {'model': z + 1}
        elif kind == 'down':
            sem, to = zsend.at[0, ss // 2, zs, part], {'model': z - 1}
        elif kind == 'x':
            sem, to = xsend.at[zs, part], {'stage': net.s_across}
        else:
            sem, to = csend.at[ss // 2, zs, part], {'stage': net.s_sibling}
        return net.send(src, slot(ss, zs, part), sem, recv.at[ss, zs, part], to)

    def arrive(ss, zs, part):
        go('c', ss, zs, part).wait_recv()

    def source(ss, d, part):
        return own.at[parts[part]] if d == 0 and ss is s else None

    def pass_on(ss, d, side, part, act):
        zs, ok = side_of(z, n_model, d, side)
        src = source(ss, d, part)
        for kind in ('up', 'down'):
            if d and kind != ('up' if side == 0 else 'down'):
                continue
            room = (z < n_model - 1) if kind == 'up' else (z > 0)
            when_all([ok, room], lambda: act(go(kind, ss, zs, part, src)))
        def rest():
            if part < last:
                act(go('x', ss, zs, part, src))
            act(go('c', ss, zs, part, src))
        when_all([ok], rest)

    def across(d, side, part, act):
        zs, ok = side_of(z, n_model, d, side)
        when_all([ok], lambda: act(go('c', net.s_across, zs, part)))

    def start(copy):
        copy.start()

    def end(copy):
        copy.wait_send()

    def sides(d):
        return range(2 if d else 1)

    def take_across(d):
        for part in range(last):
            for side in sides(d):
                zs, ok = side_of(z, n_model, d, side)
                when_all([ok], lambda: arrive(net.s_across, zs, part))
                across(d, side, part, start)

    n_block = new.shape[0] * n_model
    width = own.shape[1]
    few = 128

    def fetch(t):
        slot_of = lax.rem(t, 2)
        return pltpu.make_async_copy(new.at[lax.rem(t, n_block) // n_model, lax.rem(t, n_model)], wbuf.at[slot_of], wsem.at[slot_of])

    own[...] = acts[...]
    fetch(0).start()
    for n, (base, count, ready) in enumerate(groups):
        def block(t, _, base=base, count=count):
            fetch(t).wait()

            @pl.when(t + 1 < n_block * len(groups))
            def _():
                fetch(t + 1).start()

            turn = lax.rem(t, n_model)

            @pl.when(turn == 0)
            def _():
                total[...] = jnp.zeros(total.shape, F32)

            held = wbuf.at[lax.rem(t, 2)]
            up_w = held[:, 0].reshape(width, width)
            down_w = held[:, 1].reshape(width, width)
            ahead = dot(own[base:base + few, :], up_w)
            for r in range(count // few):
                pre = ahead
                if (r + 1) * few < count:
                    ahead = dot(own[base + (r + 1) * few:base + (r + 2) * few, :], up_w)
                total[r * few:(r + 1) * few, :] += dot(gelu_parts(pre)[0].astype(BF16), down_w)

            @pl.when(turn == n_model - 1)
            def _():
                own[base:base + count, :] = (own[base:base + count, :].astype(F32) + total[:count, :]).astype(BF16)

            return 0

        lax.fori_loop(n * n_block, (n + 1) * n_block, block, 0)
        if last in ready:
            first = go('x', s, z, last, own.at[parts[last]])
            first.start()
        for part in ready:
            pass_on(s, 0, 0, part, start)
    mine = pltpu.make_async_copy(own, out.at[s * n_model + z], local.at[0])
    mine.start()
    arrive(net.s_across, z, last)
    pass_on(net.s_across, 0, 0, last, start)
    for d in range(1, n_model):
        for part in range(last):
            for side in sides(d):
                zs, ok = side_of(z, n_model, d, side)
                when_all([ok], lambda: arrive(s, zs, part))
                pass_on(s, d, side, part, start)
        for ss in (s, net.s_across):
            for side in sides(d):
                zs, ok = side_of(z, n_model, d, side)
                when_all([ok], lambda: arrive(ss, zs, last))
                pass_on(ss, d, side, last, start)
        take_across(d - 1)
    take_across(n_model - 1)
    for ss in (net.s_sibling, lax.rem(net.s_sibling + 2, 4)):
        for zs in range(n_model):
            for part in range(last + 1):
                arrive(ss, zs, part)
    first.wait_send()
    for d in range(n_model):
        for side in sides(d):
            for part in range(last + 1):
                pass_on(s, d, side, part, end)
            for part in range(last):
                across(d, side, part, end)
            pass_on(net.s_across, d, side, last, end)
    mine.wait()


def forward_out(acts, new):
    n_stage, n_model, n_data, n_mat, half, width = new.shape
    rows = acts.shape[0]
    unit = rows // 64
    pieces = ((8 * unit, 12 * unit), (20 * unit, 12 * unit), (32 * unit, 12 * unit), (44 * unit, 10 * unit), (54 * unit, 10 * unit), (0, 8 * unit))
    groups = ((0, rows // 2, (5, 0, 1)), (rows // 2, rows // 2, (2, 3, 4)))
    n_part = len(pieces)
    return pl.pallas_call(
        functools.partial(out_kernel, n_model, pieces, groups),
        out_shape=jax.ShapeDtypeStruct((n_stage * n_model, rows, width), BF16),
        in_specs=[VMEM_SPEC, ANY_SPEC],
        out_specs=ANY_SPEC,
        scratch_shapes=[
            pltpu.VMEM((rows, width), BF16), pltpu.VMEM((rows // 2, width), F32), pltpu.VMEM((2, n_data, n_mat, half, width), BF16), DMA((2,)),
            DMA((2, 2, n_model, n_part)), DMA((n_model, n_part)), DMA((2, n_model, n_part)),
            DMA((n_stage, n_model, n_part)), DMA((1,)),
        ],
        compiler_params=pltpu.CompilerParams(has_side_effects=True, vmem_limit_bytes=20 * 1024 * 1024),
        name='forward_out',
    )(acts, new)


def store_kernel(src, dst, sems):
    n_copy = sems.shape[0]
    step = src.shape[0] // n_copy
    copies = [pltpu.make_async_copy(src.at[pl.ds(k * step, step)], dst.at[pl.ds(k * step, step)], sems.at[k]) for k in range(n_copy)]
    for copy in copies:
        copy.start()
    for copy in copies:
        copy.wait()


def store_out(rows):
    return pl.pallas_call(
        store_kernel,
        out_shape=jax.ShapeDtypeStruct(rows.shape, rows.dtype),
        in_specs=[VMEM_SPEC],
        out_specs=ANY_SPEC,
        scratch_shapes=[DMA((8,))],
        compiler_params=pltpu.CompilerParams(vmem_limit_bytes=4 * 1024 * 1024),
        name='store_out',
    )(rows)


def solution(mesh):
    n_stage = mesh.shape['stage']
    n_data = mesh.shape['data']
    n_model = mesh.shape['model']
    swap = [(0, 1), (1, 0)]
    up_spec = P('stage', None, 'model')
    down_spec = P('stage', 'model', None)
    row_spec = P(None, 'data', None)
    in_specs = (up_spec, down_spec, up_spec, down_spec, up_spec, down_spec, P('data', 'stage', None, 'model'), P('data', 'stage', 'model', None), P('stage', 'data', None), P('data', None), row_spec, P(None), P(None))
    out_specs = (up_spec, down_spec, up_spec, down_spec, up_spec, down_spec, row_spec)

    def device_step(w_up, w_down, m_up, m_down, v_up, v_down, g_up, g_down, acts_last, grad_out, x_next, learn_rate, max_norm):
        stage_id = lax.axis_index('stage')
        model_id = lax.axis_index('model')
        data_id = lax.axis_index('data')
        acts_in = acts_last[0]
        w_up, w_down, m_up, m_down, v_up, v_down = (t[0] for t in (w_up, w_down, m_up, m_down, v_up, v_down))
        g_up, g_down = g_up[0, 0], g_down[0, 0]
        d_model, ff_local = w_up.shape
        half = d_model // n_data
        up_bf = w_up.astype(BF16)
        down_bf = w_down.astype(BF16)

        def half_of(arr, which):
            return lax.dynamic_slice_in_dim(arr, which * half, half, 0)

        own = jnp.stack([up_bf, down_bf]).reshape(2, n_data, half, d_model)
        mean, norm_tile = backward_all(own, acts_in, grad_out, g_up, g_down, n_stage, n_data, n_model)
        mean_up, mean_down = mean[0], mean[1]
        norm_sq = jnp.sum(norm_tile)
        clip = jnp.minimum(1.0, max_norm[0] / (jnp.sqrt(norm_sq) + NORM_EPS))
        step_rate = learn_rate[0]

        up_half = adamw_update(half_of(w_up, data_id), half_of(m_up, data_id), half_of(v_up, data_id), clip * mean_up, step_rate)[0]
        down_half = adamw_update(half_of(w_down, data_id), half_of(m_down, data_id), half_of(v_down, data_id), clip * mean_down, step_rate)[0]
        new = gather_weights(jnp.stack([up_half.astype(BF16), down_half.astype(BF16)]), n_stage, n_model, n_data)

        new, mean_up, mean_down = lax.optimization_barrier((new, mean_up, mean_down))
        other_up = lax.ppermute(mean_up, 'data', swap)
        other_down = lax.ppermute(mean_down, 'data', swap)

        def join(mine, other):
            first = jnp.where(data_id == 0, mine, other)
            second = jnp.where(data_id == 0, other, mine)
            return jnp.concatenate([first, second], axis=0)

        up_w, up_m, up_v = adamw_update(w_up, m_up, v_up, clip * join(mean_up, other_up), step_rate)
        down_w, down_m, down_v = adamw_update(w_down, m_down, v_down, clip * join(mean_down, other_down), step_rate)

        acts_cur = lax.dynamic_index_in_dim(x_next, stage_id * n_model + model_id, 0, keepdims=False)
        y_next = store_out(forward_out(acts_cur, new))
        return (up_w[None], down_w[None], up_m[None], down_m[None], up_v[None], down_v[None], y_next)

    return jax.shard_map(device_step, mesh=mesh, in_specs=in_specs, out_specs=out_specs, check_vma=False)
```
